256 devices in a mesh: rep: 1, r: 32 (over y, z), s: 8 (over x, core).
Axes of the slice: x: 4, y: 4, z: 8, core: 2. Of those that a mesh axis runs over, the one named last changes fastest.
Arguments:
- x: bfloat16 [256, 2048, 1024], P(('rep', 'r', 's'))
- dy: bfloat16 [256, 2048, 1024], P(('rep', 'r', 's'))
- w_gate: bfloat16 [2, 1024, 3200], P(None, 's')
- w_up: bfloat16 [2, 1024, 3200], P(None, 's')
- w_down: bfloat16 [2, 3200, 1024], P(None, 's')
- m_w_gate: float32 [2, 1024, 3200], P(None, 's')
- m_w_up: float32 [2, 1024, 3200], P(None, 's')
- m_w_down: float32 [2, 3200, 1024], P(None, 's')
- v_w_gate: float32 [2, 1024, 3200], P(None, 's')
- v_w_up: float32 [2, 1024, 3200], P(None, 's')
- v_w_down: float32 [2, 3200, 1024], P(None, 's')
Outputs:
- output 1: bfloat16 [2, 1024, 3200], P('rep', 's')
- output 2: bfloat16 [2, 1024, 3200], P('rep', 's')
- output 3: bfloat16 [2, 3200, 1024], P('rep', 's')
- output 4: float32 [2, 1024, 3200], P('rep', 's')
- output 5: float32 [2, 1024, 3200], P('rep', 's')
- output 6: float32 [2, 3200, 1024], P('rep', 's')
- output 7: float32 [2, 1024, 3200], P('rep', 's')
- output 8: float32 [2, 1024, 3200], P('rep', 's')
- output 9: float32 [2, 3200, 1024], P('rep', 's')
All inputs are finite; a program needn't handle non-finite values.
Results may differ from the reference program's by a relative error of at most 0.022.
Values are sent between devices in bfloat16 or wider.
A program may use at most 768 MiB of HBM per device.

```python
import jax
import jax.numpy as jnp
from jax import lax

SEQUENCES = 256
TOKENS = 2048
D = 1024
FF = 3200
LAYERS = 2
NAMES = ("w_gate", "w_up", "w_down")
SHAPES = {"w_gate": (LAYERS, D, FF), "w_up": (LAYERS, D, FF), "w_down": (LAYERS, FF, D)}


def bump(key, n, height):
    away = (jnp.arange(n, dtype=jnp.int32) - jax.random.randint(key, (), 0, n, jnp.int32)) % n
    return jnp.where(away < n // 8, height, 1.0)


def together(key, own, strength):
    shared = jax.random.normal(key, own.shape[1:], jnp.float32)
    return (own + strength * shared) * lax.rsqrt(1 + strength * strength)


def setup_inputs(seed: int = 0, part: int = 0) -> dict:
    kx, kdy, ka, kb, kz, kf, kh, kl, *keys = jax.random.split(jax.random.key(seed), 8 + 3 * len(NAMES))
    kx, kdy, ka, kb = (jax.random.fold_in(k, part) for k in (kx, kdy, ka, kb))
    kw, km, kv = (keys[i::3] for i in range(3))
    shape = (SEQUENCES, TOKENS, D)
    much_x, much_dy = jax.random.uniform(kz, (2,), jnp.float32, 0.0, 1.0)
    loud = 2.0 ** jax.random.uniform(jax.random.fold_in(kz, 1), (), jnp.float32, -1.0, 2.0)
    layers = 2.0 ** jax.random.uniform(kl, (LAYERS, 1, 1), jnp.float32, -1.0, 1.0)
    x = together(ka, jax.random.normal(kx, shape, jnp.float32), much_x) * bump(kf, D, 4.0)
    dy = together(kb, jax.random.normal(kdy, shape, jnp.float32), much_dy)
    drawn = {"x": x.astype(jnp.bfloat16), "dy": (loud * dy * (SEQUENCES * TOKENS) ** -0.5).astype(jnp.bfloat16)}
    for key, name in zip(kw, NAMES, strict=True):
        w = jax.random.normal(key, SHAPES[name], jnp.float32) * SHAPES[name][1] ** -0.5
        drawn[name] = (w * {"w_gate": 1.0, "w_up": bump(kh, FF, 4.0), "w_down": layers}[name]).astype(jnp.bfloat16)
    for key, name in zip(km, NAMES, strict=True):
        drawn[f"m_{name}"] = 0.1 * jax.random.normal(key, SHAPES[name], jnp.float32)
    for key, name in zip(kv, NAMES, strict=True):
        drawn[f"v_{name}"] = loud * loud * jax.random.uniform(key, SHAPES[name], jnp.float32, 0.05, 0.15)
    return drawn


def matmul(a, w):
    return jnp.dot(a, w, preferred_element_type=jnp.float32).astype(jnp.bfloat16)


def normed(h):
    wide = h.astype(jnp.float32)
    scale = lax.rsqrt(jnp.mean(wide**2, -1, keepdims=True) + 1e-6)
    return (wide * scale).astype(jnp.bfloat16)


def layer(h, w):
    a = normed(h)
    gate = jnp.dot(a, w["w_gate"], preferred_element_type=jnp.float32)
    up = jnp.dot(a, w["w_up"], preferred_element_type=jnp.float32)
    return h + matmul((jax.nn.silu(gate) * up).astype(jnp.bfloat16), w["w_down"])


def adamw(w, m, v, g):
    m = 0.9 * m + 0.1 * g
    v = 0.95 * v + 0.05 * g * g
    step = m * lax.rsqrt(v + 1e-8) + 0.1 * w
    return (w - 0.02 * step).astype(jnp.bfloat16), m, v


def stack(weights, h):
    return lax.scan(lambda h, w: (layer(h, w), None), h, weights)[0]


def reference(x, dy, w_gate, w_up, w_down, m_w_gate, m_w_up, m_w_down, v_w_gate, v_w_up, v_w_down):
    weights = dict(zip(NAMES, (w_gate, w_up, w_down), strict=True))

    def take(so_far, sequence):
        h, by_y = sequence
        _, back = jax.vjp(lambda w: stack(w, h), weights)
        return jax.tree.map(lambda total, term: total + term.astype(jnp.float32), so_far, back(by_y)[0]), None

    none_yet = {name: jnp.zeros(w.shape, jnp.float32) for name, w in weights.items()}
    by_weights, _ = lax.scan(take, none_yet, (x, dy))
    gradients = [by_weights[name].astype(jnp.bfloat16).astype(jnp.float32) for name in NAMES]
    new = [
        adamw(w.astype(jnp.float32), m, v, g)
        for w, m, v, g in zip((w_gate, w_up, w_down), (m_w_gate, m_w_up, m_w_down), (v_w_gate, v_w_up, v_w_down), gradients, strict=True)
    ]
    return tuple(one[which] for which in range(3) for one in new)
```

```python
import jax
import jax.numpy as jnp
from jax import lax
from jax.experimental import pallas as pl
from jax.experimental.pallas import tpu as pltpu
from jax.sharding import PartitionSpec as P

BF, F32 = jnp.bfloat16, jnp.float32
NN, NT = (((1,), (0,)), ((), ())), (((1,), (1,)), ((), ()))
DMA, V, S = pltpu.SemaphoreType.DMA, pltpu.VMEM, jax.ShapeDtypeStruct
ANY = pl.BlockSpec(memory_space=pl.ANY)
LIMIT = 67_043_328
LAYERS, CORES, NX, NY, NZ = 2, 2, 4, 4, 8
SHARDS = NX * CORES
T, D, F = 2048, 1024, 3200
LANES, W, HALF, GROUP = 128, 256, 1024, 512
TILES = -(-F // W)
LAST = TILES - 1
GR, DR = D // SHARDS, F // SHARDS
PAIR = 2
ROWS = 256


def par(i):
    return lax.rem(i, PAIR)


def seg(i, n, step=None):
    return pl.ds(pl.multiple_of(i * (n if step is None else step), n), n)


def off(j):
    return pl.multiple_of(W * j - (TILES * W - F) * (j // LAST), LANES)


def tile_cols(j):
    return pl.ds(off(j), W)


def dot(a, b, dn=NN):
    return lax.dot_general(a, b, dn, preferred_element_type=F32)


def fetch(src, dst, sem):
    return pltpu.make_async_copy(src, dst, sem)


def start(copies):
    for c in copies:
        c.start()


def done(copies):
    for c in copies:
        c.wait()


def got(copies):
    for c in copies:
        c.wait_recv()


def sent(copies):
    for c in copies:
        c.wait_send()


def norm_of(h):
    wide = h.astype(F32)
    return wide, lax.rsqrt(jnp.mean(wide * wide, -1, keepdims=True) + 1e-6)


class Place:
    def __init__(self):
        r, s = lax.axis_index("r"), lax.axis_index("s")
        self.x, self.c, self.y, self.z = s // CORES, lax.rem(s, CORES), r // NZ, lax.rem(r, NZ)
        self.me = s

    def at(self, x, y, z, c):
        return {"r": y * NZ + z, "s": x * CORES + c}

    def along(self, axis, d):
        if axis == "x":
            return self.at(lax.rem(self.x + d, NX), self.y, self.z, self.c)
        if axis == "y":
            return self.at(self.x, lax.rem(self.y + d, NY), self.z, self.c)
        return self.at(self.x, self.y, lax.rem(self.z + d, NZ), self.c)

    def sib(self):
        return self.at(self.x, self.y, self.z, 1 - self.c)

    def greet(self):
        bar = pltpu.get_barrier_semaphore()
        peers = [self.sib()] + [self.along(a, d) for a, n in SIZES.items() for d in range(1, n)]
        for q in peers:
            pl.semaphore_signal(bar, inc=1, device_id=q, device_id_type=pl.DeviceIdType.MESH)
        pl.semaphore_wait(bar, len(peers))


SIZES = {"x": NX, "y": NY, "z": NZ}


def rcopy(src, dst, ss, rs, to):
    return pltpu.make_async_remote_copy(src, dst, ss, rs, device_id=to, device_id_type=pl.DeviceIdType.MESH)


class Gather:
    def __init__(self, route, first, width, gu):
        self.route, self.first, self.width, self.gu = route, first, width, gu

    def scratch(self):
        n = SIZES[self.route] if self.route != "x" else CORES
        return [DMA((PAIR, NX)), DMA((PAIR, n, NX)), DMA((PAIR, NX)), DMA((1,))]

    def bind(self, p, refs, own, full):
        self.p, self.own, self.full = p, own, full
        self.a, self.b, self.c, self.l = refs
        return self

    def whole(self):
        return (slice(None), pl.ds(self.first, self.width))

    def piece(self):
        q, n = (self.p.y, NY) if self.route == "y" else (self.p.z, NZ)
        if self.gu:
            return (seg(q, GR // n), pl.ds(self.first, self.width))
        n = self.width // n
        return (slice(None), pl.ds(pl.multiple_of(self.first + q * n, n), n))

    def mine(self, where):
        return self.own.at[(slice(None),) + where] if self.gu else self.own.at[where]

    def block(self, s, where):
        return self.full.at[(slice(None), s) + where] if self.gu else self.full.at[(s,) + where]

    def shard(self, k):
        return CORES * lax.rem(self.p.x + k, NX) + self.p.c

    def A(self):
        where = self.whole() if self.route == "x" else self.piece()
        return [rcopy(self.mine(where), self.block(self.p.me, where), self.a.at[0, d], self.a.at[1, d], self.p.along("x", d)) for d in range(1, NX)]

    def B(self):
        out, where = [], self.piece()
        for k in range(1, NX):
            b = self.block(self.shard(k), where)
            out += [rcopy(b, b, self.b.at[0, d, k], self.b.at[1, d, k], self.p.along(self.route, d)) for d in range(1, SIZES[self.route])]
        return out

    def O(self):
        w = self.whole()
        return [rcopy(self.mine(w), self.block(self.p.me, w), self.c.at[0, 0], self.c.at[1, 0], self.p.sib())]

    def C(self):
        out = []
        for k in range(1, NX):
            b = self.block(self.shard(k), self.whole())
            out.append(rcopy(b, b, self.c.at[0, k], self.c.at[1, k], self.p.sib()))
        return out

    def local(self):
        w = self.whole()
        return [fetch(self.mine(w), self.block(self.p.me, w), self.l.at[0])]

    def go(self):
        start(self.A() + self.O() + self.local())

    def pass_on(self):
        got(self.A())
        start(self.B())

    def share(self):
        got(self.A() if self.route == "x" else self.B())
        start(self.C())

    def ready(self):
        got(self.C() + self.O())
        done(self.local())

    def finish(self):
        sent(self.A() + self.O() + self.C() + (self.B() if self.route != "x" else []))


def gu_parts():
    return [Gather(r, f, w, True) for r, f, w in (("x", 0, W), ("x", W, W), ("y", 512, 512), ("y", 1024, 512), ("y", 1536, 768), ("z", 2304, 896))]


def down_parts(first):
    return [Gather(r, f, GROUP, False) for r, f in ((first, 0), ("y", GROUP))]


def refs_of(parts, refs):
    n = len(parts[0].scratch())
    return [refs[n * i:n * i + n] for i in range(len(parts))]


class Engine:
    def __init__(self, gu, ring):
        self.gu, self.ring, self.routes = gu, ring, ("x", "y") if gu else ("x", "x")
        self.R, self.C = (GR, W) if gu else (DR, LANES)
        self.P = 32 if gu else LANES
        self.zr = self.P // (PAIR if gu else NX)

    def scratch(self):
        R, C, Q, n = self.R, self.C, self.P, self.ring
        half = (PAIR, NX, R, C) if self.gu else (NX, R, PAIR * C)
        first = [V((n, NX - 1, R, C) if r == "x" else (n, NY - 1, NX, Q, C), BF) for r in self.routes]
        then = [V((PAIR, NY * Q, C) if r == "x" else (PAIR, NX, Q, C), BF) for r in self.routes]
        part = (NZ, self.zr, LANES)
        nd = 1 if self.gu else NX
        sems = [(PAIR, nd), (PAIR, nd)]
        for k in ((PAIR, NX), (PAIR, NX), (NZ,), (NZ,), (NY,)):
            sems += [(PAIR,) + k, (n,) + k]
        return ([V((PAIR,) + half, BF), V((PAIR, PAIR, NX, R, C), BF)] + first + then
                + [V((n, PAIR, NX - 1, Q, C), BF), V((PAIR,) + part, BF), V((n,) + part, BF), V((n,) + part, BF)]
                + [V((PAIR, PAIR, Q, C) if self.gu else (PAIR, Q, PAIR * C), BF)]
                + [DMA(s) for s in sems + [(PAIR,)]])

    REFS = 24

    def bind(self, p, refs, own, src, out_at):
        self.p, self.own, self.src, self.out_at = p, own, src, out_at
        (self.rS, self.XS, a, b, ya, yb, self.R2, self.Zp, self.R3, self.ZG, self.YS,
         self.s0, self.r0, self.s1, self.r1, self.s2, self.r2, self.s3, self.r3, self.s4, self.r4, self.s5, self.r5, self.so) = refs
        self.R1, self.Y = (a, b), (ya, yb)
        if not self.gu:
            for y in self.Y:
                for k in range(PAIR):
                    y[k, DR:] = jnp.zeros((NY * self.P - DR, self.C), BF)

    def slot(self, it):
        return lax.rem(it, self.ring)

    def c0(self, it):
        k, n = par(it), (1 if self.gu else NX)
        return [rcopy(self.src(it, i), self.rS.at[k] if self.gu else self.rS.at[k, i], self.s0.at[k, i], self.r0.at[k, i], self.p.sib()) for i in range(n)]

    def ypart(self, y):
        return seg(y, self.P)

    def c1(self, it):
        k, n, p, out = par(it), self.slot(it), self.p, []
        for d in range(1, NX):
            for m, route in enumerate(self.routes):
                src = self.XS.at[k, m, lax.rem(p.x + d, NX)] if route == "x" else self.XS.at[k, m, :, self.ypart(lax.rem(p.y + d, NY))]
                out.append(rcopy(src, self.R1[m].at[n, d - 1], self.s1.at[k, m, d], self.r1.at[n, m, d], p.along(route, d)))
        return out

    def c2(self, it):
        k, n, p, out = par(it), self.slot(it), self.p, []
        for d in range(1, NX):
            for m, route in enumerate(self.routes):
                src = self.Y[m].at[k, self.ypart(lax.rem(p.y + d, NY))] if route == "x" else self.Y[m].at[k, lax.rem(p.x + d, NX)]
                out.append(rcopy(src, self.R2.at[n, m, d - 1], self.s2.at[k, m, d], self.r2.at[n, m, d], p.along("y" if route == "x" else "x", d)))
        return out

    def c3(self, it):
        k, n, p = par(it), self.slot(it), self.p
        return [rcopy(self.Zp.at[k, lax.rem(p.z + d, NZ)], self.R3.at[n, d], self.s3.at[k, d], self.r3.at[n, d], p.along("z", d)) for d in range(1, NZ)]

    def c4(self, it):
        k, n, p = par(it), self.slot(it), self.p
        b = self.ZG.at[n, p.z]
        return [rcopy(b, b, self.s4.at[k, d], self.r4.at[n, d], p.along("z", d)) for d in range(1, NZ)]

    def c5(self, it, src, dst):
        k, n = par(it), self.slot(it)
        return [rcopy(src, dst, self.s5.at[k, d], self.r5.at[n, d], self.p.along("y", d)) for d in range(1, NY)]

    def out(self, it, f):
        for cond, src, dst in self.out_at(it):
            @pl.when(cond)
            def _():
                f(src, dst)

    def left(self, it, k):
        if k < 5:
            return sent((self.c0, self.c1, self.c2, self.c3, self.c4)[k](it))

        def f(src, dst):
            sent(self.c5(it, src, dst))
            fetch(src, dst, self.so.at[par(it)]).wait()
        self.out(it, f)

    def free(self, it, k):
        @pl.when(it >= PAIR)
        def _():
            self.left(it - PAIR, k)

    def S0(self, it):
        start(self.c0(it))

    def S1(self, it):
        k, C = par(it), self.C
        got(self.c0(it))
        self.free(it, 1)

        def add(xx, _):
            for m in range(PAIR):
                other = self.rS[k, m, xx] if self.gu else self.rS[k, xx, :, m * C:m * C + C]
                self.XS[k, m, xx] = (self.own(it, m, xx).astype(F32) + other.astype(F32)).astype(BF)
            return 0
        lax.fori_loop(0, NX, add, 0)
        start(self.c1(it))

    def S2(self, it):
        k, n, p = par(it), self.slot(it), self.p
        got(self.c1(it))
        self.free(it, 2)
        for m, route in enumerate(self.routes):
            t = (self.XS[k, m, p.x] if route == "x" else self.XS[k, m, :, self.ypart(p.y)]).astype(F32)
            for d in range(NX - 1):
                t = t + self.R1[m][n, d].astype(F32)
            if route == "x":
                self.Y[m][k, :self.R] = t.astype(BF)
            else:
                self.Y[m][k] = t.astype(BF)
        start(self.c2(it))

    def S3(self, it):
        k, n, p = par(it), self.slot(it), self.p
        got(self.c2(it))
        self.free(it, 3)
        for m, route in enumerate(self.routes):
            t = (self.Y[m][k, self.ypart(p.y)] if route == "x" else self.Y[m][k, p.x]).astype(F32)
            for d in range(NY - 1):
                t = t + self.R2[n, m, d].astype(F32)
            t = t.astype(BF)
            for q in range(NX):
                self.Zp[k, m * NX + q] = t[self.quarter(q)]
        start(self.c3(it))

    def quarter(self, q):
        z = self.zr
        if not self.gu:
            return (slice(z * q, z * q + z), slice(None))
        a, b = z * (q // PAIR), LANES * (q % PAIR)
        return (slice(a, a + z), slice(b, b + LANES))

    def S4(self, it):
        k, n, p = par(it), self.slot(it), self.p
        got(self.c3(it))
        self.free(it, 4)
        t = self.Zp[k, p.z].astype(F32)
        for d in range(1, NZ):
            t = t + self.R3[n, d].astype(F32)
        self.ZG[n, p.z] = t.astype(BF)
        start(self.c4(it))

    def S5(self, it):
        k, n = par(it), self.slot(it)
        got(self.c4(it))
        self.free(it, 5)
        for q in range(NZ):
            m, (a, b) = q // NX, self.quarter(q % NX)
            if self.gu:
                self.YS[k, m, a, b] = self.ZG[n, q]
            else:
                self.YS[k, a, m * LANES:m * LANES + LANES] = self.ZG[n, q]

        def f(src, dst):
            start(self.c5(it, src, dst) + [fetch(src, dst, self.so.at[k])])
        self.out(it, f)

    def S6(self, it):
        self.out(it, lambda src, dst: got(self.c5(it, src, dst)))

    def stage(self, k, there, it):
        @pl.when(there)
        def _():
            (self.S0, self.S1, self.S2, self.S3, self.S4, self.S5, self.S6)[k](it)

    def finish(self, items):
        for it in range(items - PAIR, items):
            for k in range(6):
                self.left(jnp.int32(it), k)


OFFS = (0, 1, 3, 5, 7, 9, 11)
LATER = (6, 5, 4, 3, 2)
WIDE_STEPS = NORM_STEPS = 4
AT_DOWN1 = TILES
AT_NORM = AT_DOWN1 + WIDE_STEPS
AT_DOWN0 = AT_NORM + NORM_STEPS
AT_TILES0 = AT_DOWN0 + WIDE_STEPS
STEPS = AT_TILES0 + TILES + OFFS[-1]
DN_STRIDE, DN_EACH = 2, D // W
DN_ITEMS = LAYERS * DN_EACH


def gu_item(u):
    v = lax.max(u, 0)
    return ((u >= 0) & (v < TILES)) | ((v >= AT_TILES0) & (v < AT_TILES0 + TILES)), v - (AT_TILES0 - TILES) * (v // AT_TILES0)


def dn_item(u):
    v = lax.max(u - AT_NORM, 0)
    return (u >= AT_NORM) & (lax.rem(v, DN_STRIDE) == 0) & (v < DN_STRIDE * DN_ITEMS), v // DN_STRIDE


class Down:
    def __init__(self, p, act_hs, dhT, h, ab, buf, town, s_a, s_o, s_t):
        self.p, self.act_hs, self.dhT, self.h, self.ab, self.buf, self.town = p, act_hs, dhT, h, ab, buf, town
        self.s_a, self.s_o, self.s_t = s_a, s_o, s_t

    def run(self, n, i):
        def load(q):
            return fetch(self.act_hs[n].at[q], self.ab.at[par(q)], self.s_a.at[par(q)])

        def store(q):
            return fetch(self.buf, self.h.at[n, tile_cols(q)], self.s_o.at[0])
        lo, each = 3 * i + lax.min(i, 1), 3 + (i == 0).astype(jnp.int32)

        def step(q, _):
            @pl.when(q == 0)
            def _():
                load(q).start()

            @pl.when(q + 1 < TILES)
            def _():
                load(q + 1).start()
            load(q).wait()
            t = dot(self.dhT[...], self.ab[par(q)]).astype(BF).T

            @pl.when(q > lo)
            def _():
                store(q - 1).wait()
            self.buf[...] = t
            store(q).start()
            return 0
        lax.fori_loop(lo, lo + each, step, 0)
        store(lo + each - 1).wait()

    def block(self, it, k, c):
        return self.h.at[it // DN_EACH, pl.ds(pl.multiple_of(DR * (CORES * k + c), 16), DR), seg(lax.rem(it, DN_EACH), W)]

    def src(self, it, k):
        return self.block(it, k, 1 - self.p.c)

    def mine(self, it):
        return [fetch(self.block(it, k, self.p.c), self.town.at[k], self.s_t.at[k]) for k in range(NX)]

    def own(self, it, m, xx):
        return self.town[xx, :, m * LANES:m * LANES + LANES]

    def hook(self, eng, i):
        for k in LATER:
            eng.stage(k, *dn_item(i - OFFS[k]))
        there, it = dn_item(i - OFFS[1])

        @pl.when(there)
        def _():
            done(self.mine(it))
            eng.S1(it)
        there0, it0 = dn_item(i)

        @pl.when(there0)
        def _():
            eng.free(it0, 0)
            start(self.mine(it0))
            eng.S0(it0)


class Sums:
    def __init__(self):
        self.gu, self.dn = Engine(True, 4), Engine(False, 2)

    def scratch(self):
        return [V((PAIR, PAIR, NX, CORES, GR, W), BF)] + self.gu.scratch() + self.dn.scratch()

    def bind(self, p, refs, gu_h, dn_h, down):
        n = Engine.REFS
        self.t, self.down = refs[0], down

        def gu_out(it):
            l, j, r, e = 1 - it // TILES, lax.rem(it, TILES), seg(p.y, 32), self.gu.YS.at[par(it)]
            return [(j < LAST, e, gu_h.at[:, l, r, seg(j, W)]), (j == LAST, e.at[:, :, LANES:], gu_h.at[:, l, r, pl.ds(F - LANES, LANES)])]

        def dn_out(it):
            return [(it >= 0, self.dn.YS.at[par(it)], dn_h.at[1 - it // DN_EACH, seg(p.y, LANES), seg(lax.rem(it, DN_EACH), W)])]
        self.gu.bind(p, refs[1:1 + n], lambda it, m, xx: self.t[par(it), m, xx, p.c], lambda it, k: self.t.at[par(it), :, :, 1 - p.c], gu_out)
        self.dn.bind(p, refs[1 + n:], down.own, down.src, dn_out)

    def put(self, it, m, aT, t):
        self.t[par(it), m] = dot(aT, t).astype(BF).reshape(NX, CORES, GR, W)

    def loop(self, tile1, put1, norm, before0, tile0, put0):
        def when(i, first, n, f):
            @pl.when((i >= first) & (i < first + n))
            def _():
                f(i - first)

        def step(i, _):
            for k in LATER:
                self.gu.stage(k, *gu_item(i - OFFS[k]))
            self.down.hook(self.dn, i)
            when(i, AT_DOWN1, WIDE_STEPS, lambda j: self.down.run(0, j))
            when(i, AT_NORM, NORM_STEPS, norm)
            when(i, AT_DOWN0 - 1, 1, before0)
            when(i, AT_DOWN0, WIDE_STEPS, lambda j: self.down.run(1, j))
            when(i, 0, TILES, tile1)
            when(i, AT_TILES0, TILES, tile0)
            self.gu.stage(1, *gu_item(i - OFFS[1]))
            when(i, 0, TILES, put1)
            when(i, AT_TILES0, TILES, put0)
            self.gu.stage(0, *gu_item(i))
            return 0
        lax.fori_loop(0, STEPS, step, 0)
        self.gu.finish(LAYERS * TILES)
        self.dn.finish(DN_ITEMS)


def hidden(d, g, u):
    sg = jax.nn.sigmoid(g)
    si = g * sg
    return si * u, d * u * (sg + si * (1 - sg)), d * si


def halves(part):
    lax.fori_loop(0, T // HALF, lambda i, _: (part(seg(i, HALF)), 0)[1], 0, unroll=True)


def stream(n, load, store, work):
    start(load(0))

    def step(i, _):
        @pl.when(i + 1 < n)
        def _():
            start(load(i + 1))
        done(load(i))

        @pl.when(i >= PAIR)
        def _():
            done(store(i - PAIR))
        work(i)
        start(store(i))
        return 0
    lax.fori_loop(0, n, step, 0)
    for i in range(n - PAIR, n):
        done(store(i))


def fa_parts():
    return gu_parts(), down_parts("x"), down_parts("y"), [Gather("x", 0, GROUP, True)]


def fa_kernel(*refs):
    (x_h, dy_h, wg_h, wu_h, wd_h, gu0_h, d0_h, d1_h, head_h, g_h, u_h, act_h, h1_h, a1_h, a1T_h, a0T_h, dyT_h,
     own0, own1, ownd, a, wd, act, wg, wu, gb, ub, xb, hb, ab, atb, s_own, s_w, s_b, s_act, s_x, s_o, s_wd), rest = refs[:38], refs[38:]
    p = Place()
    groups = fa_parts()
    every = [part for g in groups for part in g]
    for part, r, (own, full) in zip(every, refs_of(every, rest), [(own0, gu0_h)] * 6 + [(ownd.at[0], d0_h)] * 2 + [(ownd.at[1], d1_h)] * 2 + [(own1, head_h)]):
        part.bind(p, r, own, full)
    (x0, x1, y0, y1, y2, z0), (d0x, d0y), (d1a, d1b), (head,) = groups
    owns = [fetch(w.at[0], own0.at[k], s_own.at[k, 0]) for k, w in enumerate((wg_h, wu_h))]
    owns += [fetch(w.at[1, :, pl.ds(0, GROUP)], own1.at[k], s_own.at[k, 1]) for k, w in enumerate((wg_h, wu_h))]
    owns += [fetch(wd_h.at[k], ownd.at[k], s_own.at[CORES, k]) for k in range(LAYERS)]
    start(owns)
    p.greet()
    done(owns)
    for part in (y0, z0, x0, y1, x1, y2, d0y, d1a, d1b, d0x, head):
        part.go()
    n = T // GROUP

    def cut(i):
        return seg(i, GROUP)

    def first(i):
        wide, scale = norm_of(xb[par(i)])
        t = (wide * scale).astype(BF)
        a[cut(i)] = t
        atb[par(i)] = t.T

    def turn(i):
        atb[par(i)] = xb[par(i)].T

    def load(h):
        return lambda i: [fetch(h.at[cut(i)], xb.at[par(i)], s_x.at[par(i)])]

    def turned(h):
        return lambda i: [fetch(atb.at[par(i)], h.at[:, cut(i)], s_o.at[CORES, par(i)])]
    stream(n, load(x_h), turned(a0T_h), first)
    stream(n, load(dy_h), turned(dyT_h), turn)

    def wts(j):
        return [fetch(gu0_h.at[k, :, :, tile_cols(j)], w.at[par(j)], s_w.at[k, par(j)]) for k, w in enumerate((wg, wu))]

    def outs(j):
        return [fetch(b.at[par(j)], h.at[j], s_b.at[k, par(j)]) for k, (b, h) in enumerate(((gb, g_h), (ub, u_h)))]

    events = {
        0: [y0.pass_on, z0.pass_on, x0.share, x0.ready],
        1: [y1.pass_on, x1.share, x1.ready],
        2: [y2.pass_on, y0.share, y0.ready],
        4: [d0y.pass_on, y1.share, y1.ready],
        6: [d1a.pass_on, y2.share, y2.ready],
        9: [d1b.pass_on, z0.share, d0x.share, z0.ready],
    }

    def tile(j, _):
        k = par(j)
        for n_, todo in events.items():
            @pl.when(j == n_)
            def _():
                for f in todo:
                    f()
                start(wts(j))

        @pl.when(j + 1 < TILES)
        def _():
            ahead = j >= 0
            for n_ in events:
                ahead = ahead & (j + 1 != n_)

            @pl.when(ahead)
            def _():
                start(wts(j + 1))
        done(wts(j))

        @pl.when(j >= PAIR)
        def _():
            done(outs(j - PAIR))

        def part(r):
            g, u = dot(a[r], wg[k].reshape(D, W)), dot(a[r], wu[k].reshape(D, W))
            gb[k, r], ub[k, r] = g, u
            act[j, r] = (g * jax.nn.sigmoid(g) * u).astype(BF)
        halves(part)
        start(outs(j) + [fetch(act.at[j], act_h.at[j], s_act.at[j])])
        return 0
    lax.fori_loop(0, TILES, tile, 0)
    for j in range(TILES - PAIR, TILES):
        done(outs(j))
    d0y.share()
    head.share()
    d0x.ready()
    d0y.ready()
    wds = [fetch(d0_h.at[k], wd.at[pl.ds(DR * k, DR)], s_wd.at[k]) for k in range(SHARDS)]
    start(wds)
    d1a.share()
    d1b.share()
    done(wds)

    def down(i):
        k, r = par(i), cut(i)
        t = dot(act[LAST, r, LANES:], wd[F - LANES:])
        for j in range(LAST):
            t = t + dot(act[j, r], wd[W * j:W * j + W])
        h = xb[k] + t.astype(BF)
        wide, scale = norm_of(h)
        t = (wide * scale).astype(BF)
        hb[k], ab[k], atb[k] = h, t, t.T

    def finals(i):
        k, r = par(i), cut(i)
        return [fetch(hb.at[k], h1_h.at[r], s_o.at[0, k]), fetch(ab.at[k], a1_h.at[r], s_o.at[1, k]), fetch(atb.at[k], a1T_h.at[:, r], s_o.at[CORES, k])]
    stream(n, load(x_h), finals, down)
    done([fetch(act.at[j], act_h.at[j], s_act.at[j]) for j in range(TILES)])
    for part in (d1a, d1b, head):
        part.ready()
    for part in every:
        part.finish()


def params(number):
    return pltpu.CompilerParams(vmem_limit_bytes=LIMIT, collective_id=number, has_side_effects=True)


def cost(units):
    return pl.CostEstimate(flops=PAIR * units * T * D * F, bytes_accessed=LIMIT, transcendentals=T * F)


def slots(*shape, dtype=BF):
    return V((PAIR,) + shape, dtype)


def fa(x, dy, wg, wu, wd):
    tiles = lambda t: S((TILES, T, W), t)
    full = S((SHARDS, DR, D), BF)
    parts = [part for g in fa_parts() for part in g]
    return pl.pallas_call(
        fa_kernel, name="fa",
        out_shape=[S((PAIR, SHARDS, GR, F), BF), full, full, S((PAIR, SHARDS, GR, GROUP), BF), tiles(F32), tiles(F32), tiles(BF),
                   S((T, D), BF), S((T, D), BF), S((D, T), BF), S((D, T), BF), S((D, T), BF)],
        in_specs=[ANY] * 5, out_specs=[ANY] * 12,
        scratch_shapes=[slots(GR, F), slots(GR, GROUP), slots(DR, D), V((T, D), BF), V((F, D), BF), V((TILES, T, W), BF), slots(SHARDS, GR, W), slots(SHARDS, GR, W),
                        slots(T, W, dtype=F32), slots(T, W, dtype=F32), slots(GROUP, D), slots(GROUP, D), slots(GROUP, D), slots(D, GROUP),
                        DMA((3, 2)), DMA((2, 2)), DMA((2, 2)), DMA((TILES,)), DMA((2,)), DMA((3, 2)), DMA((SHARDS,))] + [s for part in parts for s in part.scratch()],
        compiler_params=params(1), cost_estimate=cost(3),
    )(x, dy, wg, wu, wd)


def bb_parts():
    return gu_parts()[2:]


def bb_kernel(*refs):
    (a_h, aT_h, dy_h, dyT_h, h_h, wg_h, wu_h, head_h, wd_h, a0T_h, act0_h, g_h, u_h, wd0_h, gu_h, dn_h, part_h, act_h, dg_h, du_h, w_h,
     a, aT, dy, dyT, da, own, wg, wu, wd, actb, dgb, dub, stage, town, hb, s_in, s_own, s_w, s_b, s_st, s_t, s_h), rest = refs[:43], refs[43:]
    p = Place()
    parts = bb_parts()
    n = sum(len(part.scratch()) for part in parts)
    for part, r in zip(parts, refs_of(parts, rest[:n])):
        part.bind(p, r, own, w_h)
    y0, y1, y2, z0 = parts
    down = Down(p, (act_h, act0_h), dyT, part_h, actb, stage, town, s_b.at[0], s_st, s_t)
    sums = Sums()
    sums.bind(p, rest[n:], gu_h, dn_h, down)
    owns = [fetch(w.at[1], own.at[k], s_own.at[k]) for k, w in enumerate((wg_h, wu_h))]
    ins = [fetch(h, v, s_in.at[k]) for k, (h, v) in enumerate(((a_h, a), (dy_h, dy), (aT_h, aT), (dyT_h, dyT)))]

    def wts(j, third):
        def of(w):
            return [fetch(w.at[k, :, :, tile_cols(j)], v.at[par(j)], s_w.at[k, par(j)]) for k, v in enumerate((wg, wu))]

        def both(f):
            @pl.when(j < PAIR)
            def _():
                f(of(head_h))

            @pl.when(j >= PAIR)
            def _():
                f(of(w_h))
            if third:
                f([fetch(wd_h.at[tile_cols(j)], wd.at[par(j)], s_w.at[CORES, par(j)])])
        return both
    bufs = ((actb, act_h), (dgb, dg_h), (dub, du_h))

    def outs(j):
        return [fetch(b.at[par(j)], h.at[j], s_b.at[k, par(j)]) for k, (b, h) in enumerate(bufs)]

    def back(j):
        return [fetch(h.at[j], b.at[par(j)], s_b.at[k, par(j)]) for k, (b, h) in enumerate(bufs) if k]
    start(owns + ins[:PAIR])
    p.greet()
    done(owns)
    for part in (y0, z0, y1, y2):
        part.go()
    start(ins[PAIR:])
    wts(jnp.int32(0), True)(start)
    da[...] = jnp.zeros(da.shape, F32)
    done(ins)
    lane = lax.broadcasted_iota(jnp.int32, (HALF, W), 1)
    events = {
        1: [y0.pass_on, z0.pass_on],
        2: [y1.pass_on, y2.pass_on, y0.share, y0.ready],
        4: [y1.share, y1.ready],
        6: [y2.share, y2.ready],
        9: [z0.share, z0.ready],
    }

    def tile(j, _):
        k = par(j)
        for n_, todo in events.items():
            @pl.when(j == n_)
            def _():
                for f in todo:
                    f()
                wts(j, True)(start)

        @pl.when(j + 1 < TILES)
        def _():
            ahead = j >= 0
            for n_ in events:
                ahead = ahead & (j + 1 != n_)

            @pl.when(ahead)
            def _():
                wts(j + 1, True)(start)
        wts(j, True)(done)

        @pl.when(j >= PAIR)
        def _():
            done(outs(j - PAIR))
        keep = lane >= LANES * (j // LAST)

        def part(r):
            g, u = dot(a[r], wg[k].reshape(D, W)), dot(a[r], wu[k].reshape(D, W))
            d = dot(dy[r], wd[k], NT).astype(BF).astype(F32)
            t, dg, du = hidden(d, g, u)
            actb[k, r] = t.astype(BF)
            dgb[k, r] = jnp.where(keep, dg, 0.0).astype(BF)
            dub[k, r] = jnp.where(keep, du, 0.0).astype(BF)
        halves(part)
        start(outs(j))
        return 0
    lax.fori_loop(0, TILES, tile, 0)
    for j in range(TILES - PAIR, TILES):
        done(outs(j))
    for part in parts:
        part.finish()

    def next_(j):
        start(back(j))
        wts(j, False)(start)
    next_(jnp.int32(0))

    def tile1(j):
        k = par(j)

        @pl.when(j + 1 < TILES)
        def _():
            next_(j + 1)
        done(back(j))
        wts(j, False)(done)

        def part(r):
            for q in range(NX):
                g, u = (w[k, CORES * q:CORES * q + CORES].reshape(W, W) for w in (wg, wu))
                da[q, r] += dot(dgb[k, r], g, NT) + dot(dub[k, r], u, NT)
        halves(part)

    def put1(j):
        sums.gu.free(j, 0)
        sums.put(j, 0, aT[...], dgb[par(j)])
        sums.put(j, 1, aT[...], dub[par(j)])

    def hs(i):
        return fetch(h_h.at[seg(i, ROWS)], hb.at[par(i)], s_h.at[par(i)])
    chunks = T // ROWS
    a0 = fetch(a0T_h, aT, s_in.at[0])

    def norm(i):
        @pl.when(i == 0)
        def _():
            a0.start()
            hs(i).start()

        def chunk(n_, _):
            r = seg(n_, ROWS)

            @pl.when(n_ + 1 < chunks)
            def _():
                hs(n_ + 1).start()
            hs(n_).wait()
            wide, scale = norm_of(hb[par(n_)])
            cut = [slice(W * q, W * q + W) for q in range(NX)]
            along = sum(jnp.sum(da[q, r] * wide[:, cut[q]], -1, keepdims=True) for q in range(NX))
            along = scale * scale * scale * (along / D)
            for q in range(NX):
                t = scale * da[q, r] - wide[:, cut[q]] * along
                dy[r, cut[q]] = (dy[r, cut[q]].astype(F32) + t).astype(BF)
            dyT[:, r] = dy[r].T
            return 0
        each = chunks // NORM_STEPS
        lax.fori_loop(i * each, i * each + each, chunk, 0)

    def tiles(j):
        k = par(j)
        return [fetch(wd0_h.at[tile_cols(j)], wd.at[k], s_w.at[CORES, k]), fetch(g_h.at[j], da.at[CORES * k], s_w.at[0, k]), fetch(u_h.at[j], da.at[CORES * k + 1], s_w.at[1, k])]

    def before0(_):
        a0.wait()
        start(tiles(jnp.int32(0)))

    def tile0(j):
        k = par(j)

        @pl.when(j + 1 < TILES)
        def _():
            start(tiles(j + 1))
        done(tiles(j))

        def part(r):
            d = dot(dy[r], wd[k], NT).astype(BF).astype(F32)
            _, dg, du = hidden(d, da[CORES * k, r], da[CORES * k + 1, r])
            dgb[0, r], dub[0, r] = dg.astype(BF), du.astype(BF)
        halves(part)
        sums.gu.free(TILES + j, 0)
        sums.put(TILES + j, 0, aT[...], dgb[0])

    def put0(j):
        sums.put(TILES + j, 1, aT[...], dub[0])
    sums.loop(tile1, put1, norm, before0, tile0, put0)


def bb(*args):
    tiles = S((TILES, T, W), BF)
    return pl.pallas_call(
        bb_kernel, name="bb",
        out_shape=[S((PAIR, LAYERS, GR, F), BF), S((LAYERS, NY * LANES, D), BF), S((LAYERS, F, D), BF), tiles, tiles, tiles, S((PAIR, SHARDS, GR, F), BF)],
        in_specs=[ANY] * len(args), out_specs=[ANY] * 7,
        scratch_shapes=[V((T, D), BF), V((D, T), BF), V((T, D), BF), V((D, T), BF), V((NX, T, W), F32), slots(GR, F), slots(SHARDS, GR, W), slots(SHARDS, GR, W), slots(W, D),
                        slots(T, W), slots(T, W), slots(T, W), V((W, D), BF), V((NX, DR, W), BF), slots(ROWS, D),
                        DMA((4,)), DMA((2,)), DMA((3, 2)), DMA((3, 2)), DMA((1,)), DMA((NX,)), DMA((2,))]
        + [s for part in bb_parts() for s in part.scratch()] + Sums().scratch(),
        compiler_params=params(2), cost_estimate=cost(12),
    )(*args)[:2]


def adamw(w, m, v, g):
    m = 0.9 * m + 0.1 * g
    v = 0.95 * v + 0.05 * g * g
    step = m * lax.rsqrt(v + 1e-8) + 0.1 * w
    return (w - 0.02 * step).astype(BF), m, v


def solution(mesh):
    def step(x, dy, *arrays):
        weights, m, v = (arrays[i:i + 3] for i in (0, 3, 6))
        x, dy = x[0], dy[0]
        _, d0, d1, head, g0, u0, act0, h1, a1, a1T, a0T, dyT = fa(x, dy, *weights)
        gu, dn = bb(a1, a1T, dy, dyT, h1, weights[0], weights[1], head, d1.reshape(F, D), a0T, act0, g0, u0, d0.reshape(F, D))
        grads = [gu[0], gu[1], dn[:, :DR]]
        new = [adamw(w.astype(F32), m_, v_, g.astype(F32)) for w, m_, v_, g in zip(weights, m, v, grads)]
        return tuple(one[k] for k in range(3) for one in new)

    states, cut = P(("rep", "r", "s"), None, None), P(None, "s", None)
    return jax.shard_map(step, mesh=mesh, in_specs=(states, states) + (cut,) * 9, out_specs=(P("rep", "s", None),) * 9, check_vma=False)
```

```python
import jax
import jax.numpy as jnp
from jax import lax
from jax.experimental import pallas as pl
from jax.experimental.pallas import tpu as pltpu
from jax.sharding import PartitionSpec as P

BF, F32 = jnp.bfloat16, jnp.float32
NN, NT = (((1,), (0,)), ((), ())), (((1,), (1,)), ((), ()))
DMA, V, S = pltpu.SemaphoreType.DMA, pltpu.VMEM, jax.ShapeDtypeStruct
ANY = pl.BlockSpec(memory_space=pl.ANY)
LIMIT = 67_043_328
LAYERS, CORES, NX, NY, NZ = 2, 2, 4, 4, 8
SHARDS = NX * CORES
T, D, F = 2048, 1024, 3200
LANES, W, HALF, GROUP = 128, 256, 1024, 512
TILES = -(-F // W)
LAST = TILES - 1
GR, DR = D // SHARDS, F // SHARDS
PAIR = 2
ROWS, HB = 256, 3


def par(i):
    return lax.rem(i, PAIR)


def seg(i, n, step=None):
    return pl.ds(pl.multiple_of(i * (n if step is None else step), n), n)


def off(j):
    return pl.multiple_of(W * j - (TILES * W - F) * (j // LAST), LANES)


def tile_cols(j):
    return pl.ds(off(j), W)


def dot(a, b, dn=NN):
    return lax.dot_general(a, b, dn, preferred_element_type=F32)


def fetch(src, dst, sem):
    return pltpu.make_async_copy(src, dst, sem)


def start(copies):
    for c in copies:
        c.start()


def done(copies):
    for c in copies:
        c.wait()


def got(copies):
    for c in copies:
        c.wait_recv()


def sent(copies):
    for c in copies:
        c.wait_send()


def norm_of(h):
    wide = h.astype(F32)
    return wide, lax.rsqrt(jnp.mean(wide * wide, -1, keepdims=True) + 1e-6)


class Place:
    def __init__(self):
        r, s = lax.axis_index("r"), lax.axis_index("s")
        self.x, self.c, self.y, self.z = s // CORES, lax.rem(s, CORES), r // NZ, lax.rem(r, NZ)
        self.me = s

    def at(self, x, y, z, c):
        return {"r": y * NZ + z, "s": x * CORES + c}

    def along(self, axis, d):
        if axis == "x":
            return self.at(lax.rem(self.x + d, NX), self.y, self.z, self.c)
        if axis == "y":
            return self.at(self.x, lax.rem(self.y + d, NY), self.z, self.c)
        return self.at(self.x, self.y, lax.rem(self.z + d, NZ), self.c)

    def sib(self):
        return self.at(self.x, self.y, self.z, 1 - self.c)

    def greet(self):
        bar = pltpu.get_barrier_semaphore()
        peers = [self.sib()] + [self.along(a, d) for a, n in SIZES.items() for d in range(1, n)]
        for q in peers:
            pl.semaphore_signal(bar, inc=1, device_id=q, device_id_type=pl.DeviceIdType.MESH)
        pl.semaphore_wait(bar, len(peers))


BOTH = 2
SIZES = {"x": NX, "y": NY, "z": NZ}


def rcopy(src, dst, ss, rs, to):
    return pltpu.make_async_remote_copy(src, dst, ss, rs, device_id=to, device_id_type=pl.DeviceIdType.MESH)


class Gather:
    def __init__(self, route, first, width, rows=None):
        self.route, self.first, self.width, self.gu = route, first, width, rows is None
        self.rows = pl.ds(0, GR) if rows is None else pl.ds(*rows)

    def scratch(self):
        return [DMA((PAIR,))] * 4 + [DMA((1,))]

    def bind(self, p, refs, own, full, base=0):
        self.p, self.own, self.full, self.base = p, own, full, base
        self.a, self.b, self.c, self.o, self.l = refs
        return self

    def whole(self):
        return (self.rows, pl.ds(self.first, self.width))

    def piece(self):
        q, n = (self.p.y, NY) if self.route == "y" else (self.p.z, NZ)
        if self.gu:
            return (seg(q, GR // n), pl.ds(self.first, self.width))
        n = self.width // n
        return (self.rows, pl.ds(pl.multiple_of(self.first + q * n, n), n))

    def mine(self, where):
        if self.base:
            where = (where[0], pl.ds(self.first - self.base, self.width))
        return self.own.at[(slice(None),) + where] if self.gu else self.own.at[where]

    def block(self, s, where):
        return self.full.at[(slice(None), s) + where] if self.gu else self.full.at[(s,) + where]

    def shard(self, k):
        return CORES * lax.rem(self.p.x + k, NX) + self.p.c

    def A(self):
        where = self.whole() if self.route == "x" else self.piece()
        return [rcopy(self.mine(where), self.block(self.p.me, where), self.a.at[0], self.a.at[1], self.p.along("x", d)) for d in range(1, NX)]

    def B(self):
        out, where = [], self.piece()
        for k in range(1, NX):
            b = self.block(self.shard(k), where)
            out += [rcopy(b, b, self.b.at[0], self.b.at[1], self.p.along(self.route, d)) for d in range(1, SIZES[self.route])]
        return out

    def O(self):
        w = self.whole()
        return [rcopy(self.mine(w), self.block(self.p.me, w), self.o.at[0], self.o.at[1], self.p.sib())]

    def C(self):
        out = []
        for k in range(1, NX):
            b = self.block(self.shard(k), self.whole())
            out.append(rcopy(b, b, self.c.at[0], self.c.at[1], self.p.sib()))
        return out

    def all_of(self, sems, where):
        b = self.block(pl.ds(0, NX - 1), where)
        return [rcopy(b, b, sems.at[0], sems.at[1], self.p.sib())]

    def all_A(self):
        return self.all_of(self.a, self.whole() if self.route == "x" else self.piece())

    def all_B(self):
        n = SIZES[self.route]
        if self.gu:
            return self.all_of(self.b, (pl.ds(0, GR // n * (n - 1)), pl.ds(self.first, self.width)))
        return self.all_of(self.b, (self.rows, pl.ds(self.first, self.width // n * (n - 1))))

    def all_C(self):
        return self.all_of(self.c, self.whole())

    def local(self):
        w = self.whole()
        return [fetch(self.mine(w), self.block(self.p.me, w), self.l.at[0])]

    def go(self):
        start(self.A() + self.O() + self.local())

    def pass_on(self):
        got(self.all_A())
        start(self.B())

    def share(self):
        got(self.all_A() if self.route == "x" else self.all_B())
        start(self.C())

    def ready(self):
        got(self.all_C() + self.O())
        done(self.local())

    def finish(self):
        sent(self.all_A() + self.O() + self.all_C() + (self.all_B() if self.route != "x" else []))


HEAD = 3 * W


def fa_parts():
    gu = [Gather(*a) for a in (("x", 0, W), ("x", W, W), ("y", 512, 512), ("y", 1024, 512), ("y", 1536, 512), ("x", 2048, W), ("z", 2304, 896))]
    d0 = [Gather(r, f, GROUP, (0, DR)) for r, f in (("x", 0), ("y", GROUP))]
    d1 = [Gather("z", 0, D, (0, 208)), Gather("y", 0, D, (208, 192))]
    return gu, d0, d1, [Gather("x", 0, HEAD)]


def bb_parts():
    return [Gather(*a) for a in (("y", HEAD, 512), ("x", 1280, 512), ("y", 1792, 512), ("z", 2304, 896))]


FRESH0, FRESH1 = (0, 1, 9), (3, 9)


def refs_of(parts, refs):
    n = len(parts[0].scratch())
    return [refs[n * i:n * i + n] for i in range(len(parts))]


class Engine:
    def __init__(self, gu, ring):
        self.gu, self.ring, self.routes = gu, ring, ("x", "y") if gu else ("x", "x")
        self.R, self.C = (GR, W) if gu else (DR, LANES)
        self.P = 32 if gu else LANES
        self.zr = self.P // (PAIR if gu else NX)
        self.lo = self.R // PAIR if gu else 208

    def scratch(self):
        R, C, Q, n = self.R, self.C, self.P, self.ring
        half = (PAIR, NX, R, C) if self.gu else (NX, R, PAIR * C)
        first = [V((n, PAIR, R, C) if r == "x" else (n, PAIR, NX, Q, C), BF) for r in self.routes]
        relay = [V((n, PAIR, self.lo, C) if r == "x" else (n, PAIR, PAIR, Q, C), BF) for r in self.routes]
        then = [V((PAIR, NY * Q, C) if r == "x" else (PAIR, NX, Q, C), BF) for r in self.routes]
        part = (NZ, self.zr, LANES)
        sems = [(PAIR,), (n,), (PAIR, PAIR), (n, PAIR), (PAIR, PAIR), (n, PAIR)] + [(PAIR,), (n,)] * 5
        return ([V((n,) + half, BF), V((n, PAIR, NX, R, C), BF)] + relay + first + then
                + [V((n, PAIR, NX - 1, Q, C), BF), V((PAIR,) + part, BF), V((n,) + part, BF), V((n,) + part, BF)]
                + [V((PAIR, PAIR, Q, C) if self.gu else (PAIR, Q, PAIR * C), BF)]
                + [DMA(s) for s in sems + [(PAIR,)]])

    REFS = 30

    def bind(self, p, refs, own, src, out_at):
        self.p, self.own, self.src, self.out_at = p, own, src, out_at
        (self.rS, self.XS, la, lb, a, b, ya, yb, self.R2, self.Zp, self.R3, self.ZG, self.YS, self.s0, self.r0, self.s1, self.r1,
         self.s2, self.r2, self.s3, self.r3, self.s4, self.r4, self.s5, self.r5, self.s6, self.r6, self.s7, self.r7, self.so) = refs
        self.RL, self.R1, self.Y = (la, lb), (a, b), (ya, yb)
        if not self.gu:
            for y in self.Y:
                for k in range(PAIR):
                    y[k, DR:] = jnp.zeros((NY * self.P - DR, self.C), BF)

    def slot(self, it):
        return lax.rem(it, self.ring)

    def c0(self, it):
        k, n_, n = par(it), self.slot(it), (1 if self.gu else NX)
        return [rcopy(self.src(it, i), self.rS.at[n_] if self.gu else self.rS.at[n_, i], self.s0.at[k], self.r0.at[n_], self.p.sib()) for i in range(n)]

    def ypart(self, y):
        return seg(y, self.P)

    def around(self, m):
        q = self.p.x if self.routes[m] == "x" else self.p.y
        return q, ((1, lax.rem(q + 1, NX)), (NX - 1, lax.rem(q + NX - 1, NX)))

    def half(self, it, m, q, i):
        n, R, lo = self.slot(it), self.R, self.lo
        if self.routes[m] == "x":
            return (n, m, q, (slice(0, lo), slice(lo, R))[i])
        return (n, m, slice(PAIR * i, PAIR * i + PAIR), self.ypart(q))

    def relayed(self, it, m, i):
        r = self.RL[m].at[self.slot(it), i]
        return r.at[pl.ds(0, (self.lo, self.R - self.lo)[i])] if self.routes[m] == "x" else r

    def c1(self, it):
        k, n, out = par(it), self.slot(it), []
        for m, route in enumerate(self.routes):
            q, near = self.around(m)
            for i, (d, _) in enumerate(near):
                out.append(rcopy(self.XS.at[self.half(it, m, lax.rem(q + CORES, NX), i)], self.relayed(it, m, i), self.s1.at[k, m], self.r1.at[n, m], self.p.along(route, d)))
        return out

    def c2(self, it):
        k, n, out = par(it), self.slot(it), []
        for m, route in enumerate(self.routes):
            for i, (d, q) in enumerate(self.around(m)[1]):
                src = self.XS.at[n, m, q] if route == "x" else self.XS.at[n, m, :, self.ypart(q)]
                out.append(rcopy(src, self.R1[m].at[n, i], self.s2.at[k, m], self.r2.at[n, m], self.p.along(route, d)))
        return out

    def c3(self, it):
        k, n, p, out = par(it), self.slot(it), self.p, []
        for d in range(1, NX):
            for m, route in enumerate(self.routes):
                src = self.Y[m].at[k, self.ypart(lax.rem(p.y + d, NY))] if route == "x" else self.Y[m].at[k, lax.rem(p.x + d, NX)]
                out.append(rcopy(src, self.R2.at[n, m, d - 1], self.s3.at[k], self.r3.at[n], p.along("y" if route == "x" else "x", d)))
        return out

    def c4(self, it):
        k, n, p = par(it), self.slot(it), self.p
        return [rcopy(self.Zp.at[k, lax.rem(p.z + d, NZ)], self.R3.at[n, d], self.s4.at[k], self.r4.at[n], p.along("z", d)) for d in range(1, NZ)]

    def c5(self, it):
        k, n, p = par(it), self.slot(it), self.p
        b = self.ZG.at[n, p.z]
        return [rcopy(b, b, self.s5.at[k], self.r5.at[n], p.along("z", d)) for d in range(1, NZ)]

    def c6(self, it, src, dst):
        k, n = par(it), self.slot(it)
        b = dst(self.p.y, None)
        return [rcopy(src, b, self.s6.at[k], self.r6.at[n], self.p.along("y", d)) for i, d in enumerate((1, NY - 1))]

    def c7(self, it, src, dst):
        k, n, out = par(it), self.slot(it), []
        for i, d in enumerate((1, NY - 1)):
            b = dst(lax.rem(self.p.y + NY - d, NY), i)
            out.append(rcopy(b, b, self.s7.at[k], self.r7.at[n], self.p.along("y", d)))
        return out

    def whole(self, it, k, dst=None):
        i, n = par(it), self.slot(it)

        def of(ref, ss, rs):
            return rcopy(ref, ref, ss, rs, self.p.sib())
        if k == 0:
            return [of(self.rS.at[n], self.s0.at[i], self.r0.at[n])]
        if k == 1:
            return [of(self.XS.at[n, m, 0] if r == "x" else self.RL[m].at[n], self.s1.at[i, m], self.r1.at[n, m]) for m, r in enumerate(self.routes)]
        if k == 2:
            return [of(self.R1[m].at[n], self.s2.at[i, m], self.r2.at[n, m]) for m in range(PAIR)]
        ref = {3: self.R2.at[n], 4: self.R3.at[n, pl.ds(1, NZ - 1)], 5: self.ZG.at[n, pl.ds(1, NZ - 1)], 6: dst and dst(0, BOTH), 7: dst and dst(self.p.y, None)}[k]
        ss, rs = {3: (self.s3, self.r3), 4: (self.s4, self.r4), 5: (self.s5, self.r5), 6: (self.s6, self.r6), 7: (self.s7, self.r7)}[k]
        return [of(ref, ss.at[i], rs.at[n])]

    def out(self, it, f):
        for cond, src, dst in self.out_at(it):
            @pl.when(cond)
            def _():
                f(src, dst)

    def left(self, it, k):
        if k < 6:
            return sent(self.whole(it, k))

        def f(src, dst):
            sent(self.whole(it, k, dst))
            if k == 6:
                fetch(src, dst(self.p.y, None), self.so.at[par(it)]).wait()
        self.out(it, f)

    def free(self, it, k):
        @pl.when(it >= PAIR)
        def _():
            self.left(it - PAIR, k)

    def S0(self, it):
        start(self.c0(it))

    def S1(self, it):
        k, n, C = par(it), self.slot(it), self.C
        got(self.whole(it, 0))
        self.free(it, 1)

        def add(xx, _):
            for m in range(PAIR):
                other = self.rS[n, m, xx] if self.gu else self.rS[n, xx, :, m * C:m * C + C]
                self.XS[n, m, xx] = (self.own(it, m, xx).astype(F32) + other.astype(F32)).astype(BF)
            return 0
        lax.fori_loop(0, NX, add, 0)
        start(self.c1(it))

    def S2(self, it):
        got(self.whole(it, 1))
        self.free(it, 2)
        for m, route in enumerate(self.routes):
            for i, (_, q) in enumerate(self.around(m)[1]):
                w, r = self.half(it, m, q, i), self.relayed(it, m, i)
                self.XS[w] = (self.XS[w].astype(F32) + r[...].astype(F32)).astype(BF)
        start(self.c2(it))

    def S3(self, it):
        k, n, p = par(it), self.slot(it), self.p
        got(self.whole(it, 2))
        self.free(it, 3)
        for m, route in enumerate(self.routes):
            t = (self.XS[n, m, p.x] if route == "x" else self.XS[n, m, :, self.ypart(p.y)]).astype(F32)
            for i in range(PAIR):
                t = t + self.R1[m][n, i].astype(F32)
            if route == "x":
                self.Y[m][k, :self.R] = t.astype(BF)
            else:
                self.Y[m][k] = t.astype(BF)
        start(self.c3(it))

    def S4(self, it):
        k, n, p = par(it), self.slot(it), self.p
        got(self.whole(it, 3))
        self.free(it, 4)
        for m, route in enumerate(self.routes):
            t = (self.Y[m][k, self.ypart(p.y)] if route == "x" else self.Y[m][k, p.x]).astype(F32)
            for d in range(NY - 1):
                t = t + self.R2[n, m, d].astype(F32)
            t = t.astype(BF)
            for q in range(NX):
                self.Zp[k, m * NX + q] = t[self.quarter(q)]
        start(self.c4(it))

    def quarter(self, q):
        z = self.zr
        if not self.gu:
            return (slice(z * q, z * q + z), slice(None))
        a, b = z * (q // PAIR), LANES * (q % PAIR)
        return (slice(a, a + z), slice(b, b + LANES))

    def S5(self, it):
        k, n, p = par(it), self.slot(it), self.p
        got(self.whole(it, 4))
        self.free(it, 5)
        t = self.Zp[k, p.z].astype(F32)
        for d in range(1, NZ):
            t = t + self.R3[n, d].astype(F32)
        self.ZG[n, p.z] = t.astype(BF)
        start(self.c5(it))

    def S6(self, it):
        k, n = par(it), self.slot(it)
        got(self.whole(it, 5))
        self.free(it, 6)
        for q in range(NZ):
            m, (a, b) = q // NX, self.quarter(q % NX)
            if self.gu:
                self.YS[k, m, a, b] = self.ZG[n, q]
            else:
                self.YS[k, a, m * LANES:m * LANES + LANES] = self.ZG[n, q]

        def f(src, dst):
            start(self.c6(it, src, dst) + [fetch(src, dst(self.p.y, None), self.so.at[k])])
        self.out(it, f)

    def S7(self, it):
        self.free(it, 7)

        def f(src, dst):
            got(self.whole(it, 6, dst))
            start(self.c7(it, src, dst))
        self.out(it, f)

    def S8(self, it):
        self.out(it, lambda src, dst: got(self.whole(it, 7, dst)))

    def stage(self, k, there, it):
        @pl.when(there)
        def _():
            (self.S0, self.S1, self.S2, self.S3, self.S4, self.S5, self.S6, self.S7, self.S8)[k](it)

    def finish(self, items):
        for it in range(items - PAIR, items):
            for k in range(8):
                self.left(jnp.int32(it), k)


OFFS = (0, 2, 4, 6, 8, 10, 12, 14, 16)
LATER = (8, 7, 6, 5, 4, 3, 2)
WIDE_STEPS = 4
AT_DOWN1 = TILES
AT_DOWN0 = AT_DOWN1 + WIDE_STEPS
AT_TILES0 = AT_DOWN0 + WIDE_STEPS
STEPS = AT_TILES0 + TILES + OFFS[-1]
DN_STRIDE, DN_EACH = 3, D // W
DN_ITEMS = LAYERS * DN_EACH


def gu_item(u):
    v = lax.max(u, 0)
    return ((u >= 0) & (v < TILES)) | ((v >= AT_TILES0) & (v < AT_TILES0 + TILES)), v - (AT_TILES0 - TILES) * (v // AT_TILES0)


def dn_item(u):
    v = lax.max(u - AT_DOWN0, 0)
    w = v - DN_EACH
    there = (v < DN_EACH) | ((lax.rem(v, DN_STRIDE) == 0) & (w < DN_STRIDE * DN_EACH))
    return (u >= AT_DOWN0) & there, lax.min(v, DN_EACH) + lax.max(w, 0) // DN_STRIDE


class Down:
    def __init__(self, p, act_hs, dhTs, h, ab, buf, town, s_a, s_o, s_t):
        self.p, self.act_hs, self.dhTs, self.h, self.ab, self.buf, self.town = p, act_hs, dhTs, h, ab, buf, town
        self.s_a, self.s_o, self.s_t = s_a, s_o, s_t

    def run(self, n, i, loads=None, work=None):
        def store(q, k):
            return fetch(self.buf.at[k], self.h.at[n, tile_cols(q)], self.s_o.at[k])

        def run(pairs, ab, other, nxt):
            q = PAIR * nxt - PAIR
            self.load(n, q, ab).wait()

            @pl.when(nxt <= LAST // PAIR)
            def _():
                self.load(n, PAIR * nxt, other).start()

            @pl.when(q > 0)
            def _():
                for k in range(PAIR):
                    store(q - PAIR + k, k).wait()
            chunks = [nxt - 1] + ([nxt] if pairs < PAIR else [])
            if work:
                loads(chunks)
            for k in range(pairs):
                self.buf[k] = dot(self.dhTs[n][...], ab[k + PAIR - pairs]).astype(BF).T
            if work:
                for c in chunks:
                    work(c)
            for k in range(pairs):
                store(q + k, k).start()

        @pl.when(i < LAST // CORES // CORES)
        def _():
            run(PAIR, self.ab[0], self.ab[1], PAIR * i + 1)
            run(PAIR, self.ab[1], self.ab[0], PAIR * i + 2)

        @pl.when(i == LAST // CORES // CORES)
        def _():
            run(1, self.ab[0], self.ab[1], PAIR * i + 1)
            store(LAST, 0).wait()

    def load(self, n, q, ab):
        return fetch(self.act_hs[n].at[pl.ds(q - q // LAST, PAIR)], ab, self.s_a.at[0])

    def first(self, n):
        self.load(n, jnp.int32(0), self.ab[0]).start()

    def block(self, it, k, c):
        return self.h.at[it // DN_EACH, pl.ds(pl.multiple_of(DR * (CORES * k + c), 16), DR), seg(lax.rem(it, DN_EACH), W)]

    def src(self, it, k):
        return self.block(it, k, 1 - self.p.c)

    def mine(self, it):
        return [fetch(self.block(it, k, self.p.c), self.town.at[par(it), k], self.s_t.at[par(it)]) for k in range(NX)]

    def own(self, it, m, xx):
        return self.town[par(it), xx, :, m * LANES:m * LANES + LANES]

    def hook(self, eng, i):
        for k in LATER:
            eng.stage(k, *dn_item(i - OFFS[k]))
        there, it = dn_item(i - OFFS[1])

        @pl.when(there)
        def _():
            fetch(eng.rS.at[0], self.town.at[0], self.s_t.at[par(it)]).wait()
            eng.S1(it)
        there0, it0 = dn_item(i)

        @pl.when(there0)
        def _():
            eng.free(it0, 0)
            start(self.mine(it0))
            eng.S0(it0)


TERMS = 3


class Sums:
    def __init__(self):
        self.gu, self.dn = Engine(True, 4), Engine(False, 4)

    def scratch(self):
        return [V((TERMS, PAIR, NX, CORES, GR, W), BF)] + self.gu.scratch() + self.dn.scratch()

    def bind(self, p, refs, gu_h, dn_h, down):
        n = Engine.REFS
        self.t, self.down = refs[0], down

        def gu_out(it):
            l, j, e = 1 - it // TILES, lax.rem(it, TILES), self.gu.YS.at[par(it)]

            def to(cols):
                def at(y, half):
                    if half == BOTH:
                        return gu_h.at[:, l, pl.ds(0, 64), cols]
                    return gu_h.at[pl.ds(0, CORES) if half is None else pl.ds(half, 1), l, seg(y, 32), cols]
                return at
            return [(j < LAST, e, to(seg(j, W))), (j == LAST, e.at[:, :, LANES:], to(pl.ds(F - LANES, LANES)))]

        def dn_out(it):
            def to(y, half):
                if half == BOTH:
                    r = pl.ds(0, CORES * LANES)
                else:
                    r = seg(y, LANES) if half is None else seg(CORES * y + half, LANES // CORES)
                return dn_h.at[1 - it // DN_EACH, r, seg(lax.rem(it, DN_EACH), W)]
            return [(it >= 0, self.dn.YS.at[par(it)], to)]
        self.gu.bind(p, refs[1:1 + n], lambda it, m, xx: self.t[lax.rem(it, TERMS), m, xx, p.c], lambda it, k: self.t.at[lax.rem(it, TERMS), :, :, 1 - p.c], gu_out)
        self.dn.bind(p, refs[1 + n:], down.own, down.src, dn_out)

    def put(self, it, m, aT, t):
        self.t[lax.rem(it, TERMS), m] = dot(aT, t).astype(BF).reshape(NX, CORES, GR, W)

    def loop(self, tile1, beside, after1, before0, tile0):
        def when(i, first, n, f):
            @pl.when((i >= first) & (i < first + n))
            def _():
                f(i - first)

        def step(i, _):
            for k in LATER + (1,):
                self.gu.stage(k, *gu_item(i - OFFS[k]))
            self.down.hook(self.dn, i)
            when(i, AT_DOWN1, WIDE_STEPS, lambda j: self.down.run(0, j, *beside))
            when(i, AT_DOWN1 - 1, 1, lambda _: self.down.first(0))
            when(i, AT_DOWN0, 1, lambda _: self.down.first(1))
            when(i, AT_DOWN0, 1, after1)
            when(i, AT_TILES0 - 1, 1, before0)
            when(i, AT_DOWN0, WIDE_STEPS, lambda j: self.down.run(1, j))
            when(i, 0, TILES, tile1)
            when(i, AT_TILES0, TILES, tile0)
            self.gu.stage(0, *gu_item(i))
            return 0
        lax.fori_loop(0, STEPS, step, 0)
        self.gu.finish(LAYERS * TILES)
        self.dn.finish(DN_ITEMS)


def sigmoid(g):
    return 0.5 * jnp.tanh(0.5 * g) + 0.5


def hidden(d, g, u):
    sg = sigmoid(g)
    si = g * sg
    return si * u, d * u * (sg + si * (1 - sg)), d * si


def halves(part):
    lax.fori_loop(0, T // HALF, lambda i, _: (part(seg(i, HALF)), 0)[1], 0, unroll=True)


def stream(n, load, store, work):
    start(load(0))

    def step(i, _):
        @pl.when(i + 1 < n)
        def _():
            start(load(i + 1))
        done(load(i))

        @pl.when(i >= PAIR)
        def _():
            done(store(i - PAIR))
        work(i)
        start(store(i))
        return 0
    lax.fori_loop(0, n, step, 0)
    for i in range(n - PAIR, n):
        done(store(i))


def fa_kernel(*refs):
    (x_h, dy_h, wg_h, wu_h, wd_h, gu0_h, d0_h, d1_h, head_h, g_h, u_h, act_h, h1_h, a1_h, a1T_h, a0T_h, dyT_h,
     own0, own1, ownd, a, wd, act, wg, wu, gb, ub, xb, hb, ab, atb, s_own, s_w, s_b, s_act, s_x, s_o, s_wd, s_dy), rest = refs[:39], refs[39:]
    p = Place()
    groups = fa_parts()
    every = [part for g in groups for part in g]
    for part, r, (own, full) in zip(every, refs_of(every, rest), [(own0, gu0_h)] * len(groups[0]) + [(ownd.at[0], d0_h)] * 2 + [(ownd.at[1], d1_h)] * 2 + [(own1, head_h)]):
        part.bind(p, r, own, full)
    (x0, x1, y0, y1, y2, x2, z0), (d0x, d0y), (d1z, d1y), (head,) = groups
    owns = [fetch(w.at[0], own0.at[k], s_own.at[k, 0]) for k, w in enumerate((wg_h, wu_h))]
    owns += [fetch(w.at[1, :, pl.ds(0, HEAD)], own1.at[k], s_own.at[k, 1]) for k, w in enumerate((wg_h, wu_h))]
    owns += [fetch(wd_h.at[k], ownd.at[k], s_own.at[CORES, k]) for k in range(LAYERS)]
    start(owns)
    p.greet()
    done(owns)
    for part in (y0, z0, x0, y1, x1, y2, x2, d0y, d1z, d1y, d0x, head):
        part.go()
    n = T // GROUP

    def cut(i):
        return seg(i, GROUP)

    def first(i):
        wide, scale = norm_of(xb[par(i)])
        t = (wide * scale).astype(BF)
        a[cut(i)] = t
        atb[par(i)] = t.T

    def dys(i):
        return fetch(dy_h.at[seg(i, GROUP)], hb.at[i % PAIR], s_dy.at[i % PAIR])

    def turn(i):
        def f():
            dys(i).wait()
            if i >= PAIR:
                turned(dyT_h)(i - PAIR)[0].wait()
            atb[i % PAIR] = hb[i % PAIR].T
            start(turned(dyT_h)(i))
            if i + PAIR < n:
                dys(i + PAIR).start()
        return f

    def load(h):
        return lambda i: [fetch(h.at[cut(i)], xb.at[par(i)], s_x.at[par(i)])]

    def turned(h):
        return lambda i: [fetch(atb.at[par(i)], h.at[:, cut(i)], s_o.at[CORES, par(i)])]
    for i in range(PAIR):
        dys(i).start()
    stream(n, load(x_h), turned(a0T_h), first)

    def wts(j):
        return [fetch(gu0_h.at[k, :, :, tile_cols(j)], w.at[par(j)], s_w.at[k, par(j)]) for k, w in enumerate((wg, wu))]

    def outs(j):
        return [fetch(b.at[par(j)], h.at[j], s_b.at[k, par(j)]) for k, (b, h) in enumerate(((gb, g_h), (ub, u_h)))]

    events = {
        0: [y0.pass_on, z0.pass_on, turn(0), turn(1), x0.share, x0.ready, y1.pass_on],
        1: [turn(2), y0.share, x1.share, x1.ready, y2.pass_on, y0.ready],
        2: [y1.share],
        3: [d0y.pass_on, y1.ready],
        4: [d1z.pass_on, d1y.pass_on, y2.share],
        5: [turn(3), x2.share, y2.ready],
        7: [x2.ready],
        8: [z0.share],
        9: [d0x.share, d0y.share, z0.ready],
        11: [d0x.ready, d0y.ready],
    }

    def tile(j, _):
        k = par(j)
        for n_, todo in events.items():
            @pl.when(j == n_)
            def _():
                for f in todo:
                    f()
                if n_ in FRESH0:
                    start(wts(j))

        @pl.when(j + 1 < TILES)
        def _():
            ahead = j >= 0
            for n_ in FRESH0:
                ahead = ahead & (j + 1 != n_)

            @pl.when(ahead)
            def _():
                start(wts(j + 1))
        done(wts(j))

        @pl.when(j == LAST - 1)
        def _():
            start(wds)

        @pl.when(j >= PAIR)
        def _():
            done(outs(j - PAIR))

        def part(r):
            g, u = dot(a[r], wg[k].reshape(D, W)), dot(a[r], wu[k].reshape(D, W))
            gb[k, r], ub[k, r] = g, u
            act[j, r] = (g * sigmoid(g) * u).astype(BF)
        halves(part)
        start(outs(j) + [fetch(act.at[j], act_h.at[j], s_act.at[j])])
        return 0
    wds = [fetch(d0_h.at[k], wd.at[pl.ds(DR * k, DR)], s_wd.at[k]) for k in range(SHARDS)]
    lax.fori_loop(0, TILES, tile, 0)
    for j in range(TILES - PAIR, TILES):
        done(outs(j))
    for i in range(n - PAIR, n):
        done(turned(dyT_h)(i))
    done(wds)

    def down(i):
        k, r = par(i), cut(i)

        @pl.when(i == 0)
        def _():
            d1y.share()

        @pl.when(i == 1)
        def _():
            d1z.share()
            head.share()
        t = dot(act[LAST, r, LANES:], wd[F - LANES:])
        for j in range(LAST):
            t = t + dot(act[j, r], wd[W * j:W * j + W])
        h = xb[k] + t.astype(BF)
        wide, scale = norm_of(h)
        t = (wide * scale).astype(BF)
        hb[k], ab[k], atb[k] = h, t, t.T

    def finals(i):
        k, r = par(i), cut(i)
        return [fetch(hb.at[k], h1_h.at[r], s_o.at[0, k]), fetch(ab.at[k], a1_h.at[r], s_o.at[1, k]), fetch(atb.at[k], a1T_h.at[:, r], s_o.at[CORES, k])]
    stream(n, load(x_h), finals, down)
    done([fetch(act.at[j], act_h.at[j], s_act.at[j]) for j in range(TILES)])
    for part in (d1z, d1y, head):
        part.ready()
    for part in every:
        part.finish()


def params(number):
    return pltpu.CompilerParams(vmem_limit_bytes=LIMIT, collective_id=number, has_side_effects=True)


def cost(units):
    return pl.CostEstimate(flops=PAIR * units * T * D * F, bytes_accessed=LIMIT, transcendentals=T * F)


def slots(*shape, dtype=BF):
    return V((PAIR,) + shape, dtype)


def fa(x, dy, wg, wu, wd):
    tiles = lambda t: S((TILES, T, W), t)
    full = S((SHARDS, DR, D), BF)
    parts = [part for g in fa_parts() for part in g]
    return pl.pallas_call(
        fa_kernel, name="fa",
        out_shape=[S((PAIR, SHARDS, GR, F), BF), full, full, S((PAIR, SHARDS, GR, HEAD), BF), tiles(F32), tiles(F32), tiles(BF),
                   S((T, D), BF), S((T, D), BF), S((D, T), BF), S((D, T), BF), S((D, T), BF)],
        in_specs=[ANY] * 5, out_specs=[ANY] * 12,
        scratch_shapes=[slots(GR, F), slots(GR, HEAD), slots(DR, D), V((T, D), BF), V((F, D), BF), V((TILES, T, W), BF), slots(SHARDS, GR, W), slots(SHARDS, GR, W),
                        slots(T, W, dtype=F32), slots(T, W, dtype=F32), slots(GROUP, D), slots(GROUP, D), slots(GROUP, D), slots(D, GROUP),
                        DMA((3, 2)), DMA((2, 2)), DMA((2, 2)), DMA((TILES,)), DMA((2,)), DMA((3, 2)), DMA((SHARDS,)), DMA((2,))] + [s for part in parts for s in part.scratch()],
        compiler_params=params(1), cost_estimate=cost(3),
    )(x, dy, wg, wu, wd)


def bb_kernel(*refs):
    (a_h, aT_h, dy_h, dyT_h, h_h, wg_h, wu_h, head_h, wd_h, a0T_h, act0_h, g_h, u_h, wd0_h, gu_h, dn_h, part_h, act_h, dg_h, du_h, w_h,
     a, aT, dy, dyT, da, own, wg, wu, wd, actb, dgb, dub, stage, town, hb, s_in, s_own, s_w, s_b, s_st, s_t, s_h), rest = refs[:43], refs[43:]
    p = Place()
    parts = bb_parts()
    n = sum(len(part.scratch()) for part in parts)
    for part, r in zip(parts, refs_of(parts, rest[:n])):
        part.bind(p, r, own, w_h, HEAD)
    y0, x1, y2, z0 = parts
    down = Down(p, (act_h, act0_h), (dyT, aT), part_h, (actb, dgb), stage, town, s_b.at[0], s_st, s_t)
    sums = Sums()
    sums.bind(p, rest[n:], gu_h, dn_h, down)
    owns = [fetch(w.at[1, :, pl.ds(HEAD, F - HEAD)], own.at[k], s_own.at[k]) for k, w in enumerate((wg_h, wu_h))]
    ins = [fetch(h, v, s_in.at[k]) for k, (h, v) in enumerate(((a_h, a), (dy_h, dy), (aT_h, aT), (dyT_h, dyT)))]

    def wts(j, third):
        def of(w):
            return [fetch(w.at[k, :, :, tile_cols(j)], v.at[par(j)], s_w.at[k, par(j)]) for k, v in enumerate((wg, wu))]

        def both(f):
            @pl.when(j < HEAD // W)
            def _():
                f(of(head_h))

            @pl.when(j >= HEAD // W)
            def _():
                f(of(w_h))
            if third:
                f([fetch(wd_h.at[tile_cols(j)], wd.at[par(j)], s_w.at[CORES, par(j)])])
        return both
    bufs = ((actb, act_h), (dgb, dg_h), (dub, du_h))

    def outs(j):
        return [fetch(b.at[par(j)], h.at[j], s_b.at[k, par(j)]) for k, (b, h) in enumerate(bufs)]

    def back(j):
        return [fetch(h.at[j], b.at[par(j)], s_b.at[k, par(j)]) for k, (b, h) in enumerate(bufs) if k]
    start(owns + ins[:PAIR])
    wts(jnp.int32(0), True)(start)
    start(ins[PAIR:])
    da[...] = jnp.zeros(da.shape, F32)
    p.greet()
    done(owns)
    for part in (y0, z0, y2, x1):
        part.go()
    done(ins[:PAIR])
    lane = lax.broadcasted_iota(jnp.int32, (HALF, W), 1)
    events = {
        1: [y0.pass_on, z0.pass_on],
        2: [y2.pass_on],
        3: [y0.share, y0.ready],
        4: [x1.share, x1.ready],
        5: [y2.share],
        6: [y2.ready],
        8: [z0.share],
        9: [z0.ready],
    }

    def tile(j, _):
        k = par(j)
        for n_, todo in events.items():
            @pl.when(j == n_)
            def _():
                for f in todo:
                    f()
                if n_ in FRESH1:
                    wts(j, True)(start)

        @pl.when(j + 1 < TILES)
        def _():
            ahead = j >= 0
            for n_ in FRESH1:
                ahead = ahead & (j + 1 != n_)

            @pl.when(ahead)
            def _():
                wts(j + 1, True)(start)
        wts(j, True)(done)

        @pl.when(j >= PAIR)
        def _():
            done(outs(j - PAIR))
        keep = lane >= LANES * (j // LAST)

        def part(r):
            g, u = dot(a[r], wg[k].reshape(D, W)), dot(a[r], wu[k].reshape(D, W))
            d = dot(dy[r], wd[k], NT).astype(BF).astype(F32)
            t, dg, du = hidden(d, g, u)
            actb[k, r] = t.astype(BF)
            dgb[k, r] = jnp.where(keep, dg, 0.0).astype(BF)
            dub[k, r] = jnp.where(keep, du, 0.0).astype(BF)
        halves(part)
        start(outs(j))
        return 0
    lax.fori_loop(0, TILES, tile, 0)
    for j in range(TILES - PAIR, TILES):
        done(outs(j))
    done(ins[PAIR:])
    for part in parts:
        part.finish()

    def next_(j):
        start(back(j))
        wts(j, False)(start)
    next_(jnp.int32(0))
    for i in range(PAIR):
        fetch(h_h.at[seg(i, ROWS)], hb.at[i], s_h.at[i]).start()

    def tile1(j):
        k = par(j)

        @pl.when(j + 1 < TILES)
        def _():
            next_(j + 1)
        done(back(j))
        wts(j, False)(done)

        def part(r):
            for q in range(NX):
                g, u = (w[k, CORES * q:CORES * q + CORES].reshape(W, W) for w in (wg, wu))
                da[q, r] += dot(dgb[k, r], g, NT) + dot(dub[k, r], u, NT)
        sums.gu.free(j, 0)
        halves(part)
        sums.put(j, 0, aT[...], dgb[par(j)])
        sums.put(j, 1, aT[...], dub[par(j)])

    def hs(i):
        return fetch(h_h.at[seg(i, ROWS)], hb.at[lax.rem(i, HB)], s_h.at[lax.rem(i, HB)])

    def norm_loads(todo):
        for i in todo:
            hs(i).wait()
        for i in todo:
            @pl.when(i + PAIR < T // ROWS)
            def _():
                hs(i + PAIR).start()

    def norm(i):
        r, k = seg(i, ROWS), lax.rem(i, HB)
        wide, scale = norm_of(hb[k])
        cut = [slice(W * q, W * q + W) for q in range(NX)]
        along = sum(jnp.sum(da[q, r] * wide[:, cut[q]], -1, keepdims=True) for q in range(NX))
        along = scale * scale * scale * (along / D)
        parts = [(dy[r, cut[q]].astype(F32) + (scale * da[q, r] - wide[:, cut[q]] * along)).astype(BF) for q in range(NX)]
        for q in range(NX):
            a[r, cut[q]] = parts[q]
            aT[cut[q], r] = parts[q].T
    a0 = fetch(a0T_h, dyT, s_in.at[0])

    def after1(_):
        a0.start()

    def tiles(j):
        k = par(j)
        return [fetch(wd0_h.at[tile_cols(j)], wd.at[k], s_w.at[CORES, k]), fetch(g_h.at[j], da.at[CORES * k], s_w.at[0, k]), fetch(u_h.at[j], da.at[CORES * k + 1], s_w.at[1, k])]

    def before0(_):
        a0.wait()
        start(tiles(jnp.int32(0)))

    def tile0(j):
        k = par(j)

        @pl.when(j + 1 < TILES)
        def _():
            start(tiles(j + 1))
        done(tiles(j))

        def part(r):
            d = dot(a[r], wd[k], NT).astype(BF).astype(F32)
            _, dg, du = hidden(d, da[CORES * k, r], da[CORES * k + 1, r])
            dgb[0, r], dub[0, r] = dg.astype(BF), du.astype(BF)
        sums.gu.free(TILES + j, 0)
        halves(part)
        sums.put(TILES + j, 0, dyT[...], dgb[0])
        sums.put(TILES + j, 1, dyT[...], dub[0])
    sums.loop(tile1, (norm_loads, norm), after1, before0, tile0)


def bb(*args):
    tiles = S((TILES, T, W), BF)
    return pl.pallas_call(
        bb_kernel, name="bb",
        out_shape=[S((PAIR, LAYERS, GR, F), BF), S((LAYERS, NY * LANES, D), BF), S((LAYERS, F, D), BF), tiles, tiles, tiles, S((PAIR, SHARDS, GR, F), BF)],
        in_specs=[ANY] * len(args), out_specs=[ANY] * 7,
        scratch_shapes=[V((T, D), BF), V((D, T), BF), V((T, D), BF), V((D, T), BF), V((NX, T, W), F32), slots(GR, F - HEAD), slots(SHARDS, GR, W), slots(SHARDS, GR, W), slots(W, D),
                        slots(T, W), slots(T, W), slots(T, W), slots(W, D), slots(NX, DR, W), V((HB, ROWS, D), BF),
                        DMA((4,)), DMA((2,)), DMA((3, 2)), DMA((3, 2)), DMA((2,)), DMA((NX,)), DMA((HB,))]
        + [s for part in bb_parts() for s in part.scratch()] + Sums().scratch(),
        compiler_params=params(2), cost_estimate=cost(12),
    )(*args)[:2]


def adamw(w, m, v, g):
    m = 0.9 * m + 0.1 * g
    v = 0.95 * v + 0.05 * g * g
    step = m * lax.rsqrt(v + 1e-8) + 0.1 * w
    return (w - 0.02 * step).astype(BF), m, v


def solution(mesh):
    def step(x, dy, *arrays):
        weights, m, v = (arrays[i:i + 3] for i in (0, 3, 6))
        x, dy = x[0], dy[0]
        _, d0, d1, head, g0, u0, act0, h1, a1, a1T, a0T, dyT = fa(x, dy, *weights)
        gu, dn = bb(a1, a1T, dy, dyT, h1, weights[0], weights[1], head, d1.reshape(F, D), a0T, act0, g0, u0, d0.reshape(F, D))
        grads = [gu[0], gu[1], dn[:, :DR]]
        new = [adamw(w.astype(F32), m_, v_, g.astype(F32)) for w, m_, v_, g in zip(weights, m, v, grads)]
        return tuple(one[k] for k in range(3) for one in new)

    states, cut = P(("rep", "r", "s"), None, None), P(None, "s", None)
    return jax.shard_map(step, mesh=mesh, in_specs=(states, states) + (cut,) * 9, out_specs=(P("rep", "s", None),) * 9, check_vma=False)
```

```python
import jax
import jax.numpy as jnp
from jax import lax
from jax.experimental import pallas as pl
from jax.experimental.pallas import tpu as pltpu
from jax.sharding import PartitionSpec as P

BF, F32 = jnp.bfloat16, jnp.float32
NN, NT = (((1,), (0,)), ((), ())), (((1,), (1,)), ((), ()))
DMA, V, S = pltpu.SemaphoreType.DMA, pltpu.VMEM, jax.ShapeDtypeStruct
ANY = pl.BlockSpec(memory_space=pl.ANY)
LIMIT = 67_043_328
LAYERS, CORES, NX, NY, NZ = 2, 2, 4, 4, 8
SHARDS = NX * CORES
T, D, F = 2048, 1024, 3200
LANES, W, HALF, GROUP = 128, 256, 1024, 512
TILES = -(-F // W)
LAST = TILES - 1
GR, DR = D // SHARDS, F // SHARDS
PAIR = 2
ROWS, HB = 256, 3


def par(i):
    return lax.rem(i, PAIR)


def seg(i, n, step=None):
    return pl.ds(pl.multiple_of(i * (n if step is None else step), n), n)


def off(j):
    return pl.multiple_of(W * j - (TILES * W - F) * (j // LAST), LANES)


def tile_cols(j):
    return pl.ds(off(j), W)


def dot(a, b, dn=NN):
    return lax.dot_general(a, b, dn, preferred_element_type=F32)


def fetch(src, dst, sem):
    return pltpu.make_async_copy(src, dst, sem)


def start(copies):
    for c in copies:
        c.start()


def done(copies):
    for c in copies:
        c.wait()


def got(copies):
    for c in copies:
        c.wait_recv()


def sent(copies):
    for c in copies:
        c.wait_send()


def norm_of(h):
    wide = h.astype(F32)
    return wide, lax.rsqrt(jnp.mean(wide * wide, -1, keepdims=True) + 1e-6)


class Place:
    def __init__(self):
        r, s = lax.axis_index("r"), lax.axis_index("s")
        self.x, self.c, self.y, self.z = s // CORES, lax.rem(s, CORES), r // NZ, lax.rem(r, NZ)
        self.me = s

    def at(self, x, y, z, c):
        return {"r": y * NZ + z, "s": x * CORES + c}

    def along(self, axis, d):
        if axis == "x":
            return self.at(lax.rem(self.x + d, NX), self.y, self.z, self.c)
        if axis == "y":
            return self.at(self.x, lax.rem(self.y + d, NY), self.z, self.c)
        return self.at(self.x, self.y, lax.rem(self.z + d, NZ), self.c)

    def sib(self):
        return self.at(self.x, self.y, self.z, 1 - self.c)

    def greet(self):
        bar = pltpu.get_barrier_semaphore()
        peers = [self.sib()] + [self.along(a, d) for a, n in SIZES.items() for d in range(1, n)]
        for q in peers:
            pl.semaphore_signal(bar, inc=1, device_id=q, device_id_type=pl.DeviceIdType.MESH)
        pl.semaphore_wait(bar, len(peers))


BOTH = 2
SIZES = {"x": NX, "y": NY, "z": NZ}


def rcopy(src, dst, ss, rs, to):
    return pltpu.make_async_remote_copy(src, dst, ss, rs, device_id=to, device_id_type=pl.DeviceIdType.MESH)


class Gather:
    def __init__(self, route, first, width, rows=None):
        self.route, self.first, self.width, self.gu = route, first, width, rows is None
        self.rows = pl.ds(0, GR) if rows is None else pl.ds(*rows)

    def scratch(self):
        return [DMA((PAIR,))] * 4 + [DMA((1,))]

    def bind(self, p, refs, own, full, base=0):
        self.p, self.own, self.full, self.base = p, own, full, base
        self.a, self.b, self.c, self.o, self.l = refs
        return self

    def whole(self):
        return (self.rows, pl.ds(self.first, self.width))

    def piece(self):
        q, n = (self.p.y, NY) if self.route == "y" else (self.p.z, NZ)
        if self.gu:
            return (seg(q, GR // n), pl.ds(self.first, self.width))
        n = self.width // n
        return (self.rows, pl.ds(pl.multiple_of(self.first + q * n, n), n))

    def mine(self, where):
        if self.base:
            where = (where[0], pl.ds(self.first - self.base, self.width))
        return self.own.at[(slice(None),) + where] if self.gu else self.own.at[where]

    def block(self, s, where):
        return self.full.at[(slice(None), s) + where] if self.gu else self.full.at[(s,) + where]

    def shard(self, k):
        return CORES * lax.rem(self.p.x + k, NX) + self.p.c

    def A(self):
        where = self.whole() if self.route == "x" else self.piece()
        return [rcopy(self.mine(where), self.block(self.p.me, where), self.a.at[0], self.a.at[1], self.p.along("x", d)) for d in range(1, NX)]

    def B(self):
        out, where = [], self.piece()
        for k in range(1, NX):
            b = self.block(self.shard(k), where)
            out += [rcopy(b, b, self.b.at[0], self.b.at[1], self.p.along(self.route, d)) for d in range(1, SIZES[self.route])]
        return out

    def O(self):
        w = self.whole()
        return [rcopy(self.mine(w), self.block(self.p.me, w), self.o.at[0], self.o.at[1], self.p.sib())]

    def C(self):
        out = []
        for k in range(1, NX):
            b = self.block(self.shard(k), self.whole())
            out.append(rcopy(b, b, self.c.at[0], self.c.at[1], self.p.sib()))
        return out

    def all_of(self, sems, where):
        b = self.block(pl.ds(0, NX - 1), where)
        return [rcopy(b, b, sems.at[0], sems.at[1], self.p.sib())]

    def all_A(self):
        return self.all_of(self.a, self.whole() if self.route == "x" else self.piece())

    def all_B(self):
        n = SIZES[self.route]
        if self.gu:
            return self.all_of(self.b, (pl.ds(0, GR // n * (n - 1)), pl.ds(self.first, self.width)))
        return self.all_of(self.b, (self.rows, pl.ds(self.first, self.width // n * (n - 1))))

    def all_C(self):
        return self.all_of(self.c, self.whole())

    def local(self):
        w = self.whole()
        return [fetch(self.mine(w), self.block(self.p.me, w), self.l.at[0])]

    def go(self):
        start(self.A() + self.O() + self.local())

    def pass_on(self):
        got(self.all_A())
        start(self.B())

    def share(self):
        got(self.all_A() if self.route == "x" else self.all_B())
        start(self.C())

    def ready(self):
        got(self.all_C() + self.O())
        done(self.local())

    def finish(self):
        sent(self.all_A() + self.O() + self.all_C() + (self.all_B() if self.route != "x" else []))


HEAD = 4 * W


def fa_parts():
    gu = [Gather(*a) for a in (("x", 0, W), ("x", W, W), ("y", 512, 512), ("y", 1024, 512), ("y", 1536, 512), ("x", 2048, W), ("z", 2304, 896))]
    d0 = [Gather(r, f, GROUP, (0, DR)) for r, f in (("x", 0), ("y", GROUP))]
    d1 = [Gather("z", 0, D, (0, 208)), Gather("y", 0, D, (208, 192))]
    return gu, d0, d1, [Gather("x", 0, HEAD)]


def bb_parts():
    return [Gather(*a) for a in (("y", HEAD, W), ("x", HEAD + W, 512), ("y", 1792, 512), ("z", 2304, 896))]


FRESH0, FRESH1 = (0, 1), (4, 5)


def refs_of(parts, refs):
    n = len(parts[0].scratch())
    return [refs[n * i:n * i + n] for i in range(len(parts))]


class Engine:
    def __init__(self, gu, ring):
        self.gu, self.ring, self.routes = gu, ring, ("x", "y") if gu else ("x", "x")
        self.R, self.C = (GR, W) if gu else (DR, LANES)
        self.P = 32 if gu else LANES
        self.zr = self.P // (PAIR if gu else NX)
        self.lo = self.R // PAIR if gu else 208

    def scratch(self):
        R, C, Q, n = self.R, self.C, self.P, self.ring
        half = (PAIR, NX, R, C) if self.gu else (NX, R, PAIR * C)
        first = [V((n, PAIR, R, C) if r == "x" else (n, PAIR, NX, Q, C), BF) for r in self.routes]
        relay = [V((n, PAIR, self.lo, C) if r == "x" else (n, PAIR, PAIR, Q, C), BF) for r in self.routes]
        then = [V((PAIR, NY * Q, C) if r == "x" else (PAIR, NX, Q, C), BF) for r in self.routes]
        part = (NZ, self.zr, LANES)
        sems = [(PAIR,), (n,), (PAIR, PAIR), (n, PAIR), (PAIR, PAIR), (n, PAIR)] + [(PAIR,), (n,)] * 5
        return ([V((n,) + half, BF), V((n, PAIR, NX, R, C), BF)] + relay + first + then
                + [V((n, PAIR, NX - 1, Q, C), BF), V((PAIR,) + part, BF), V((n,) + part, BF), V((n,) + part, BF)]
                + [V((PAIR, PAIR, Q, C) if self.gu else (PAIR, Q, PAIR * C), BF)]
                + [DMA(s) for s in sems + [(PAIR,)]])

    REFS = 30

    def bind(self, p, refs, own, src, out_at):
        self.p, self.own, self.src, self.out_at = p, own, src, out_at
        (self.rS, self.XS, la, lb, a, b, ya, yb, self.R2, self.Zp, self.R3, self.ZG, self.YS, self.s0, self.r0, self.s1, self.r1,
         self.s2, self.r2, self.s3, self.r3, self.s4, self.r4, self.s5, self.r5, self.s6, self.r6, self.s7, self.r7, self.so) = refs
        self.RL, self.R1, self.Y = (la, lb), (a, b), (ya, yb)
        if not self.gu:
            for y in self.Y:
                for k in range(PAIR):
                    y[k, DR:] = jnp.zeros((NY * self.P - DR, self.C), BF)

    def slot(self, it):
        return lax.rem(it, self.ring)

    def c0(self, it):
        k, n_, n = par(it), self.slot(it), (1 if self.gu else NX)
        return [rcopy(self.src(it, i), self.rS.at[n_] if self.gu else self.rS.at[n_, i], self.s0.at[k], self.r0.at[n_], self.p.sib()) for i in range(n)]

    def ypart(self, y):
        return seg(y, self.P)

    def around(self, m):
        q = self.p.x if self.routes[m] == "x" else self.p.y
        return q, ((1, lax.rem(q + 1, NX)), (NX - 1, lax.rem(q + NX - 1, NX)))

    def half(self, it, m, q, i):
        n, R, lo = self.slot(it), self.R, self.lo
        if self.routes[m] == "x":
            return (n, m, q, (slice(0, lo), slice(lo, R))[i])
        return (n, m, slice(PAIR * i, PAIR * i + PAIR), self.ypart(q))

    def relayed(self, it, m, i):
        r = self.RL[m].at[self.slot(it), i]
        return r.at[pl.ds(0, (self.lo, self.R - self.lo)[i])] if self.routes[m] == "x" else r

    def c1(self, it):
        k, n, out = par(it), self.slot(it), []
        for m, route in enumerate(self.routes):
            q, near = self.around(m)
            for i, (d, _) in enumerate(near):
                out.append(rcopy(self.XS.at[self.half(it, m, lax.rem(q + CORES, NX), i)], self.relayed(it, m, i), self.s1.at[k, m], self.r1.at[n, m], self.p.along(route, d)))
        return out

    def c2(self, it):
        k, n, out = par(it), self.slot(it), []
        for m, route in enumerate(self.routes):
            for i, (d, q) in enumerate(self.around(m)[1]):
                src = self.XS.at[n, m, q] if route == "x" else self.XS.at[n, m, :, self.ypart(q)]
                out.append(rcopy(src, self.R1[m].at[n, i], self.s2.at[k, m], self.r2.at[n, m], self.p.along(route, d)))
        return out

    def c3(self, it):
        k, n, p, out = par(it), self.slot(it), self.p, []
        for d in range(1, NX):
            for m, route in enumerate(self.routes):
                src = self.Y[m].at[k, self.ypart(lax.rem(p.y + d, NY))] if route == "x" else self.Y[m].at[k, lax.rem(p.x + d, NX)]
                out.append(rcopy(src, self.R2.at[n, m, d - 1], self.s3.at[k], self.r3.at[n], p.along("y" if route == "x" else "x", d)))
        return out

    def c4(self, it):
        k, n, p = par(it), self.slot(it), self.p
        return [rcopy(self.Zp.at[k, lax.rem(p.z + d, NZ)], self.R3.at[n, d], self.s4.at[k], self.r4.at[n], p.along("z", d)) for d in range(1, NZ)]

    def c5(self, it):
        k, n, p = par(it), self.slot(it), self.p
        b = self.ZG.at[n, p.z]
        return [rcopy(b, b, self.s5.at[k], self.r5.at[n], p.along("z", d)) for d in range(1, NZ)]

    def c6(self, it, src, dst):
        k, n = par(it), self.slot(it)
        b = dst(self.p.y, None)
        return [rcopy(src, b, self.s6.at[k], self.r6.at[n], self.p.along("y", d)) for i, d in enumerate((1, NY - 1))]

    def c7(self, it, src, dst):
        k, n, out = par(it), self.slot(it), []
        for i, d in enumerate((1, NY - 1)):
            b = dst(lax.rem(self.p.y + NY - d, NY), i)
            out.append(rcopy(b, b, self.s7.at[k], self.r7.at[n], self.p.along("y", d)))
        return out

    def whole(self, it, k, dst=None):
        i, n = par(it), self.slot(it)

        def of(ref, ss, rs):
            return rcopy(ref, ref, ss, rs, self.p.sib())
        if k == 0:
            return [of(self.rS.at[n], self.s0.at[i], self.r0.at[n])]
        if k == 1:
            return [of(self.XS.at[n, m, 0] if r == "x" else self.RL[m].at[n], self.s1.at[i, m], self.r1.at[n, m]) for m, r in enumerate(self.routes)]
        if k == 2:
            return [of(self.R1[m].at[n], self.s2.at[i, m], self.r2.at[n, m]) for m in range(PAIR)]
        ref = {3: self.R2.at[n], 4: self.R3.at[n, pl.ds(1, NZ - 1)], 5: self.ZG.at[n, pl.ds(1, NZ - 1)], 6: dst and dst(0, BOTH), 7: dst and dst(self.p.y, None)}[k]
        ss, rs = {3: (self.s3, self.r3), 4: (self.s4, self.r4), 5: (self.s5, self.r5), 6: (self.s6, self.r6), 7: (self.s7, self.r7)}[k]
        return [of(ref, ss.at[i], rs.at[n])]

    def out(self, it, f):
        for cond, src, dst in self.out_at(it):
            @pl.when(cond)
            def _():
                f(src, dst)

    def left(self, it, k):
        if k < 6:
            return sent(self.whole(it, k))

        def f(src, dst):
            sent(self.whole(it, k, dst))
            if k == 6:
                fetch(src, dst(self.p.y, None), self.so.at[par(it)]).wait()
        self.out(it, f)

    def free(self, it, k):
        @pl.when(it >= PAIR)
        def _():
            self.left(it - PAIR, k)

    def S0(self, it):
        start(self.c0(it))

    def S1(self, it):
        k, n, C = par(it), self.slot(it), self.C
        got(self.whole(it, 0))
        self.free(it, 1)

        def add(xx, _):
            for m in range(PAIR):
                other = self.rS[n, m, xx] if self.gu else self.rS[n, xx, :, m * C:m * C + C]
                self.XS[n, m, xx] = (self.own(it, m, xx).astype(F32) + other.astype(F32)).astype(BF)
            return 0
        lax.fori_loop(0, NX, add, 0)
        start(self.c1(it))

    def S2(self, it):
        got(self.whole(it, 1))
        self.free(it, 2)
        for m, route in enumerate(self.routes):
            for i, (_, q) in enumerate(self.around(m)[1]):
                w, r = self.half(it, m, q, i), self.relayed(it, m, i)
                self.XS[w] = (self.XS[w].astype(F32) + r[...].astype(F32)).astype(BF)
        start(self.c2(it))

    def S3(self, it):
        k, n, p = par(it), self.slot(it), self.p
        got(self.whole(it, 2))
        self.free(it, 3)
        for m, route in enumerate(self.routes):
            t = (self.XS[n, m, p.x] if route == "x" else self.XS[n, m, :, self.ypart(p.y)]).astype(F32)
            for i in range(PAIR):
                t = t + self.R1[m][n, i].astype(F32)
            if route == "x":
                self.Y[m][k, :self.R] = t.astype(BF)
            else:
                self.Y[m][k] = t.astype(BF)
        start(self.c3(it))

    def S4(self, it):
        k, n, p = par(it), self.slot(it), self.p
        got(self.whole(it, 3))
        self.free(it, 4)
        for m, route in enumerate(self.routes):
            t = (self.Y[m][k, self.ypart(p.y)] if route == "x" else self.Y[m][k, p.x]).astype(F32)
            for d in range(NY - 1):
                t = t + self.R2[n, m, d].astype(F32)
            t = t.astype(BF)
            for q in range(NX):
                self.Zp[k, m * NX + q] = t[self.quarter(q)]
        start(self.c4(it))

    def quarter(self, q):
        z = self.zr
        if not self.gu:
            return (slice(z * q, z * q + z), slice(None))
        a, b = z * (q // PAIR), LANES * (q % PAIR)
        return (slice(a, a + z), slice(b, b + LANES))

    def S5(self, it):
        k, n, p = par(it), self.slot(it), self.p
        got(self.whole(it, 4))
        self.free(it, 5)
        t = self.Zp[k, p.z].astype(F32)
        for d in range(1, NZ):
            t = t + self.R3[n, d].astype(F32)
        self.ZG[n, p.z] = t.astype(BF)
        start(self.c5(it))

    def S6(self, it):
        k, n = par(it), self.slot(it)
        got(self.whole(it, 5))
        self.free(it, 6)
        for q in range(NZ):
            m, (a, b) = q // NX, self.quarter(q % NX)
            if self.gu:
                self.YS[k, m, a, b] = self.ZG[n, q]
            else:
                self.YS[k, a, m * LANES:m * LANES + LANES] = self.ZG[n, q]

        def f(src, dst):
            start(self.c6(it, src, dst) + [fetch(src, dst(self.p.y, None), self.so.at[k])])
        self.out(it, f)

    def S7(self, it):
        self.free(it, 7)

        def f(src, dst):
            got(self.whole(it, 6, dst))
            start(self.c7(it, src, dst))
        self.out(it, f)

    def S8(self, it):
        self.out(it, lambda src, dst: got(self.whole(it, 7, dst)))

    def stage(self, k, there, it):
        @pl.when(there)
        def _():
            (self.S0, self.S1, self.S2, self.S3, self.S4, self.S5, self.S6, self.S7, self.S8)[k](it)

    def finish(self, items):
        for it in range(items - PAIR, items):
            for k in range(8):
                self.left(jnp.int32(it), k)


OFFS = (0, 2, 4, 6, 8, 10, 12, 14, 16)
LATER = (8, 7, 6, 5, 4, 3, 2)
WIDE_STEPS = 4
AT_DOWN1 = TILES
AT_DOWN0 = AT_DOWN1 + WIDE_STEPS
AT_TILES0 = AT_DOWN0 + WIDE_STEPS
STEPS = AT_TILES0 + TILES + OFFS[-1]
DN_STRIDE, DN_EACH = 3, D // W
DN_ITEMS = LAYERS * DN_EACH


def gu_item(u):
    v = lax.max(u, 0)
    return ((u >= 0) & (v < TILES)) | ((v >= AT_TILES0) & (v < AT_TILES0 + TILES)), v - (AT_TILES0 - TILES) * (v // AT_TILES0)


def dn_item(u):
    v = lax.max(u - AT_DOWN0, 0)
    w = v - DN_EACH
    there = (v < DN_EACH) | ((lax.rem(v, DN_STRIDE) == 0) & (w < DN_STRIDE * DN_EACH))
    return (u >= AT_DOWN0) & there, lax.min(v, DN_EACH) + lax.max(w, 0) // DN_STRIDE


class Down:
    def __init__(self, p, act_hs, dhTs, h, ab, buf, town, s_a, s_o, s_t):
        self.p, self.act_hs, self.dhTs, self.h, self.ab, self.buf, self.town = p, act_hs, dhTs, h, ab, buf, town
        self.s_a, self.s_o, self.s_t = s_a, s_o, s_t

    def run(self, n, i, loads=None, work=None):
        def store(q, k):
            return fetch(self.buf.at[k], self.h.at[n, tile_cols(q)], self.s_o.at[k])

        def run(pairs, ab, other, nxt):
            q = PAIR * nxt - PAIR
            self.load(n, q, ab).wait()

            @pl.when(nxt <= LAST // PAIR)
            def _():
                self.load(n, PAIR * nxt, other).start()

            @pl.when(q > 0)
            def _():
                for k in range(PAIR):
                    store(q - PAIR + k, k).wait()
            chunks = [nxt - 1] + ([nxt] if pairs < PAIR else [])
            if work:
                loads(chunks)
            for k in range(pairs):
                self.buf[k] = dot(self.dhTs[n][...], ab[k + PAIR - pairs]).astype(BF).T
            if work:
                for c in chunks:
                    work(c)
            for k in range(pairs):
                store(q + k, k).start()

        @pl.when(i < LAST // CORES // CORES)
        def _():
            run(PAIR, self.ab[0], self.ab[1], PAIR * i + 1)
            run(PAIR, self.ab[1], self.ab[0], PAIR * i + 2)

        @pl.when(i == LAST // CORES // CORES)
        def _():
            run(1, self.ab[0], self.ab[1], PAIR * i + 1)
            store(LAST, 0).wait()

    def load(self, n, q, ab):
        return fetch(self.act_hs[n].at[pl.ds(q - q // LAST, PAIR)], ab, self.s_a.at[0])

    def first(self, n):
        self.load(n, jnp.int32(0), self.ab[0]).start()

    def block(self, it, k, c):
        return self.h.at[it // DN_EACH, pl.ds(pl.multiple_of(DR * (CORES * k + c), 16), DR), seg(lax.rem(it, DN_EACH), W)]

    def src(self, it, k):
        return self.block(it, k, 1 - self.p.c)

    def mine(self, it):
        return [fetch(self.block(it, k, self.p.c), self.town.at[par(it), k], self.s_t.at[par(it)]) for k in range(NX)]

    def own(self, it, m, xx):
        return self.town[par(it), xx, :, m * LANES:m * LANES + LANES]

    def hook(self, eng, i):
        for k in LATER:
            eng.stage(k, *dn_item(i - OFFS[k]))
        there, it = dn_item(i - OFFS[1])

        @pl.when(there)
        def _():
            fetch(eng.rS.at[0], self.town.at[0], self.s_t.at[par(it)]).wait()
            eng.S1(it)
        there0, it0 = dn_item(i)

        @pl.when(there0)
        def _():
            eng.free(it0, 0)
            start(self.mine(it0))
            eng.S0(it0)


TERMS = 3


class Sums:
    def __init__(self):
        self.gu, self.dn = Engine(True, 4), Engine(False, 4)

    def scratch(self):
        return [V((TERMS, PAIR, NX, CORES, GR, W), BF)] + self.gu.scratch() + self.dn.scratch()

    def bind(self, p, refs, gu_h, dn_h, down):
        n = Engine.REFS
        self.t, self.down = refs[0], down

        def gu_out(it):
            l, j, e = 1 - it // TILES, lax.rem(it, TILES), self.gu.YS.at[par(it)]

            def to(cols):
                def at(y, half):
                    if half == BOTH:
                        return gu_h.at[:, l, pl.ds(0, 64), cols]
                    return gu_h.at[pl.ds(0, CORES) if half is None else pl.ds(half, 1), l, seg(y, 32), cols]
                return at
            return [(j < LAST, e, to(seg(j, W))), (j == LAST, e.at[:, :, LANES:], to(pl.ds(F - LANES, LANES)))]

        def dn_out(it):
            def to(y, half):
                if half == BOTH:
                    r = pl.ds(0, CORES * LANES)
                else:
                    r = seg(y, LANES) if half is None else seg(CORES * y + half, LANES // CORES)
                return dn_h.at[1 - it // DN_EACH, r, seg(lax.rem(it, DN_EACH), W)]
            return [(it >= 0, self.dn.YS.at[par(it)], to)]
        self.gu.bind(p, refs[1:1 + n], lambda it, m, xx: self.t[lax.rem(it, TERMS), m, xx, p.c], lambda it, k: self.t.at[lax.rem(it, TERMS), :, :, 1 - p.c], gu_out)
        self.dn.bind(p, refs[1 + n:], down.own, down.src, dn_out)

    def put(self, it, m, aT, t):
        self.t[lax.rem(it, TERMS), m] = dot(aT, t).astype(BF).reshape(NX, CORES, GR, W)

    def loop(self, tile1, beside, after1, before0, tile0):
        def when(i, first, n, f):
            @pl.when((i >= first) & (i < first + n))
            def _():
                f(i - first)

        def step(i, _):
            for k in LATER + (1,):
                self.gu.stage(k, *gu_item(i - OFFS[k]))

            @pl.when(i >= AT_DOWN0)
            def _():
                self.down.hook(self.dn, i)
            when(i, AT_DOWN1, WIDE_STEPS, lambda j: self.down.run(0, j, *beside))
            when(i, AT_DOWN1 - 1, 1, lambda _: self.down.first(0))
            when(i, AT_DOWN0 - 1, 1, lambda _: self.down.first(1))
            when(i, AT_DOWN0, 1, after1)
            when(i, AT_TILES0 - 1, 1, before0)
            when(i, AT_DOWN0, WIDE_STEPS, lambda j: self.down.run(1, j))
            when(i, 0, TILES, tile1)
            when(i, AT_TILES0, TILES, tile0)
            self.gu.stage(0, *gu_item(i))
            return 0
        lax.fori_loop(0, STEPS, step, 0)
        self.gu.finish(LAYERS * TILES)
        self.dn.finish(DN_ITEMS)


def sigmoid(g):
    return 0.5 * jnp.tanh(0.5 * g) + 0.5


def hidden(d, g, u):
    sg = sigmoid(g)
    si = g * sg
    return si * u, d * u * (sg + si * (1 - sg)), d * si


def halves(part, rows=HALF):
    lax.fori_loop(0, T // rows, lambda i, _: (part(seg(i, rows)), 0)[1], 0, unroll=True)


def stream(n, load, store, work):
    start(load(0))

    def step(i, _):
        @pl.when(i + 1 < n)
        def _():
            start(load(i + 1))
        done(load(i))

        @pl.when(i >= PAIR)
        def _():
            done(store(i - PAIR))
        work(i)
        start(store(i))
        return 0
    lax.fori_loop(0, n, step, 0)
    for i in range(n - PAIR, n):
        done(store(i))


def fa_kernel(*refs):
    (x_h, dy_h, wg_h, wu_h, wd_h, gu0_h, d0_h, d1_h, head_h, g_h, u_h, act_h, h1_h, a1_h, a1T_h, a0T_h, dyT_h,
     own0, own1, ownd, a, wd, act, wg, wu, gb, ub, xb, hb, ab, atb, s_own, s_w, s_b, s_act, s_x, s_o, s_wd, s_dy), rest = refs[:39], refs[39:]
    p = Place()
    groups = fa_parts()
    every = [part for g in groups for part in g]
    for part, r, (own, full) in zip(every, refs_of(every, rest), [(own0, gu0_h)] * len(groups[0]) + [(ownd.at[0], d0_h)] * 2 + [(ownd.at[1], d1_h)] * 2 + [(own1, head_h)]):
        part.bind(p, r, own, full)
    (x0, x1, y0, y1, y2, x2, z0), (d0x, d0y), (d1z, d1y), (head,) = groups
    owns = [fetch(w.at[0], own0.at[k], s_own.at[k, 0]) for k, w in enumerate((wg_h, wu_h))]
    owns += [fetch(w.at[1, :, pl.ds(0, HEAD)], own1.at[k], s_own.at[k, 1]) for k, w in enumerate((wg_h, wu_h))]
    owns += [fetch(wd_h.at[k], ownd.at[k], s_own.at[CORES, k]) for k in range(LAYERS)]
    start(owns)
    p.greet()
    done(owns)
    for part in (y0, z0, x0, y1, x1, y2, x2, d0y, d1z, d1y, d0x, head):
        part.go()
    n = T // GROUP

    def cut(i):
        return seg(i, GROUP)

    def first(i):
        wide, scale = norm_of(xb[par(i)])
        t = (wide * scale).astype(BF)
        a[cut(i)] = t
        atb[par(i)] = t.T

    def dys(i):
        return fetch(dy_h.at[seg(i, GROUP)], hb.at[i % PAIR], s_dy.at[i % PAIR])

    def turn(i):
        def f():
            dys(i).wait()
            if i >= PAIR:
                turned(dyT_h)(i - PAIR)[0].wait()
            atb[i % PAIR] = hb[i % PAIR].T
            start(turned(dyT_h)(i))
            if i + PAIR < n:
                dys(i + PAIR).start()
        return f

    def load(h):
        return lambda i: [fetch(h.at[cut(i)], xb.at[par(i)], s_x.at[par(i)])]

    def turned(h):
        return lambda i: [fetch(atb.at[par(i)], h.at[:, cut(i)], s_o.at[CORES, par(i)])]
    for i in range(PAIR):
        dys(i).start()
    stream(n, load(x_h), turned(a0T_h), first)

    def wts(j):
        return [fetch(gu0_h.at[k, :, :, tile_cols(j)], w.at[par(j)], s_w.at[k, par(j)]) for k, w in enumerate((wg, wu))]

    def outs(j):
        return [fetch(b.at[par(j)], h.at[j], s_b.at[k, par(j)]) for k, (b, h) in enumerate(((gb, g_h), (ub, u_h)))]

    events = {
        0: [y0.pass_on, z0.pass_on, turn(0), turn(1), x0.share, x0.ready, y1.pass_on],
        1: [turn(2), y0.share, x1.share, x1.ready, y2.pass_on, y0.ready],
        2: [y1.share],
        3: [turn(3), y1.ready],
        4: [d0y.pass_on, y2.share],
        5: [x2.share, y2.ready],
        6: [d1z.pass_on, d1y.pass_on],
        7: [x2.ready, z0.share],
        8: [z0.ready],
        9: [d0y.share],
        11: [d0x.share],
        12: [d0x.ready, d0y.ready],
    }

    def tile(j, _):
        k = par(j)
        for n_, todo in events.items():
            @pl.when(j == n_)
            def _():
                for f in todo:
                    f()
                if n_ in FRESH0:
                    start(wts(j))

        @pl.when(j + 1 < TILES)
        def _():
            ahead = j >= 0
            for n_ in FRESH0:
                ahead = ahead & (j + 1 != n_)

            @pl.when(ahead)
            def _():
                start(wts(j + 1))
        done(wts(j))

        @pl.when(j == LAST)
        def _():
            start(wds)

        @pl.when(j >= PAIR)
        def _():
            done(outs(j - PAIR))

        def part(r):
            g, u = dot(a[r], wg[k].reshape(D, W)), dot(a[r], wu[k].reshape(D, W))
            gb[k, r], ub[k, r] = g, u
            act[j, r] = (g * sigmoid(g) * u).astype(BF)
        halves(part)
        start(outs(j) + [fetch(act.at[j], act_h.at[j], s_act.at[j])])
        return 0
    wds = [fetch(d0_h.at[k], wd.at[pl.ds(DR * k, DR)], s_wd.at[k]) for k in range(SHARDS)]
    lax.fori_loop(0, TILES, tile, 0)
    for j in range(TILES - PAIR, TILES):
        done(outs(j))
    for i in range(n - PAIR, n):
        done(turned(dyT_h)(i))
    done(wds)

    def down(i):
        k, r = par(i), cut(i)

        @pl.when(i == 0)
        def _():
            d1y.share()

        @pl.when(i == 1)
        def _():
            d1z.share()

        @pl.when(i == 3)
        def _():
            head.share()
        t = dot(act[LAST, r, LANES:], wd[F - LANES:])
        for j in range(LAST):
            t = t + dot(act[j, r], wd[W * j:W * j + W])
        h = xb[k] + t.astype(BF)
        wide, scale = norm_of(h)
        t = (wide * scale).astype(BF)
        hb[k], ab[k], atb[k] = h, t, t.T

    def finals(i):
        k, r = par(i), cut(i)
        return [fetch(hb.at[k], h1_h.at[r], s_o.at[0, k]), fetch(ab.at[k], a1_h.at[r], s_o.at[1, k]), fetch(atb.at[k], a1T_h.at[:, r], s_o.at[CORES, k])]
    stream(n, load(x_h), finals, down)
    done([fetch(act.at[j], act_h.at[j], s_act.at[j]) for j in range(TILES)])
    for part in (d1z, d1y, head):
        part.ready()
    for part in every:
        part.finish()


def params(number):
    return pltpu.CompilerParams(vmem_limit_bytes=LIMIT, collective_id=number, has_side_effects=True)


def cost(units):
    return pl.CostEstimate(flops=PAIR * units * T * D * F, bytes_accessed=LIMIT, transcendentals=T * F)


def slots(*shape, dtype=BF):
    return V((PAIR,) + shape, dtype)


def fa(x, dy, wg, wu, wd):
    tiles = lambda t: S((TILES, T, W), t)
    full = S((SHARDS, DR, D), BF)
    parts = [part for g in fa_parts() for part in g]
    return pl.pallas_call(
        fa_kernel, name="fa",
        out_shape=[S((PAIR, SHARDS, GR, F), BF), full, full, S((PAIR, SHARDS, GR, HEAD), BF), tiles(F32), tiles(F32), tiles(BF),
                   S((T, D), BF), S((T, D), BF), S((D, T), BF), S((D, T), BF), S((D, T), BF)],
        in_specs=[ANY] * 5, out_specs=[ANY] * 12,
        scratch_shapes=[slots(GR, F), slots(GR, HEAD), slots(DR, D), V((T, D), BF), V((F, D), BF), V((TILES, T, W), BF), slots(SHARDS, GR, W), slots(SHARDS, GR, W),
                        slots(T, W, dtype=F32), slots(T, W, dtype=F32), slots(GROUP, D), slots(GROUP, D), slots(GROUP, D), slots(D, GROUP),
                        DMA((3, 2)), DMA((2, 2)), DMA((2, 2)), DMA((TILES,)), DMA((2,)), DMA((3, 2)), DMA((SHARDS,)), DMA((2,))] + [s for part in parts for s in part.scratch()],
        compiler_params=params(1), cost_estimate=cost(3),
    )(x, dy, wg, wu, wd)


def bb_kernel(*refs):
    (a_h, aT_h, dy_h, dyT_h, h_h, wg_h, wu_h, head_h, wd_h, a0T_h, act0_h, g_h, u_h, wd0_h, gu_h, dn_h, part_h, act_h, dg_h, du_h, w_h,
     a, aT, dy, dyT, da, own, wg, wu, wd, actb, dgb, dub, stage, town, hb, s_in, s_own, s_w, s_b, s_st, s_t, s_h), rest = refs[:43], refs[43:]
    p = Place()
    parts = bb_parts()
    n = sum(len(part.scratch()) for part in parts)
    for part, r in zip(parts, refs_of(parts, rest[:n])):
        part.bind(p, r, own, w_h, HEAD)
    y0, x1, y2, z0 = parts
    down = Down(p, (act_h, act0_h), (dyT, aT), part_h, (actb, dgb), stage, town, s_b.at[0], s_st, s_t)
    sums = Sums()
    sums.bind(p, rest[n:], gu_h, dn_h, down)
    owns = [fetch(w.at[1, :, pl.ds(HEAD, F - HEAD)], own.at[k], s_own.at[k]) for k, w in enumerate((wg_h, wu_h))]
    ins = [fetch(h, v, s_in.at[k]) for k, (h, v) in enumerate(((a_h, a), (dy_h, dy), (aT_h, aT), (dyT_h, dyT)))]

    def wts(j, third):
        def of(w):
            return [fetch(w.at[k, :, :, tile_cols(j)], v.at[par(j)], s_w.at[k, par(j)]) for k, v in enumerate((wg, wu))]

        def both(f):
            @pl.when(j < HEAD // W)
            def _():
                f(of(head_h))

            @pl.when(j >= HEAD // W)
            def _():
                f(of(w_h))
            if third:
                f([fetch(wd_h.at[tile_cols(j)], wd.at[par(j)], s_w.at[CORES, par(j)])])
        return both
    bufs = ((actb, act_h), (dgb, dg_h), (dub, du_h))

    def outs(j):
        return [fetch(b.at[par(j)], h.at[j], s_b.at[k, par(j)]) for k, (b, h) in enumerate(bufs)]

    def back(j):
        return [fetch(h.at[j], b.at[par(j)], s_b.at[k, par(j)]) for k, (b, h) in enumerate(bufs) if k]
    start(owns + ins[:PAIR])
    wts(jnp.int32(0), True)(start)
    start(ins[PAIR:])
    da[...] = jnp.zeros(da.shape, F32)
    p.greet()
    done(owns)
    for part in (y0, z0, y2, x1):
        part.go()
    done(ins[:PAIR])
    lane = lax.broadcasted_iota(jnp.int32, (HALF, W), 1)
    events = {
        1: [y0.pass_on, z0.pass_on],
        2: [y2.pass_on],
        4: [y0.share, y0.ready, x1.share],
        5: [y2.share, x1.ready],
        6: [y2.ready],
        7: [z0.share],
        8: [z0.ready],
    }

    def tile(j, _):
        k = par(j)
        for n_, todo in events.items():
            @pl.when(j == n_)
            def _():
                for f in todo:
                    f()
                if n_ in FRESH1:
                    wts(j, True)(start)

        @pl.when(j + 1 < TILES)
        def _():
            ahead = j >= 0
            for n_ in FRESH1:
                ahead = ahead & (j + 1 != n_)

            @pl.when(ahead)
            def _():
                wts(j + 1, True)(start)
        wts(j, True)(done)

        @pl.when(j >= PAIR)
        def _():
            done(outs(j - PAIR))
        keep = lane >= LANES * (j // LAST)

        def part(r):
            g, u = dot(a[r], wg[k].reshape(D, W)), dot(a[r], wu[k].reshape(D, W))
            d = dot(dy[r], wd[k], NT).astype(BF).astype(F32)
            t, dg, du = hidden(d, g, u)
            actb[k, r] = t.astype(BF)
            dgb[k, r] = jnp.where(keep, dg, 0.0).astype(BF)
            dub[k, r] = jnp.where(keep, du, 0.0).astype(BF)
        halves(part)
        start(outs(j))
        return 0
    lax.fori_loop(0, TILES, tile, 0)
    for j in range(TILES - PAIR, TILES):
        done(outs(j))
    done(ins[PAIR:])
    for part in parts:
        part.finish()

    def next_(j):
        start(back(j))
        wts(j, False)(start)
    next_(jnp.int32(0))
    for i in range(PAIR):
        fetch(h_h.at[seg(i, ROWS)], hb.at[i], s_h.at[i]).start()

    def tile1(j):
        k = par(j)

        @pl.when(j + 1 < TILES)
        def _():
            next_(j + 1)
        done(back(j))
        wts(j, False)(done)

        def part(r):
            for q in range(NX):
                g, u = (w[k, CORES * q:CORES * q + CORES].reshape(W, W) for w in (wg, wu))
                da[q, r] += dot(dgb[k, r], g, NT) + dot(dub[k, r], u, NT)
        sums.gu.free(j, 0)
        halves(part)
        sums.put(j, 0, aT[...], dgb[par(j)])
        sums.put(j, 1, aT[...], dub[par(j)])

    def hs(i):
        return fetch(h_h.at[seg(i, ROWS)], hb.at[lax.rem(i, HB)], s_h.at[lax.rem(i, HB)])

    def norm_loads(todo):
        for i in todo:
            hs(i).wait()
        for i in todo:
            @pl.when(i + PAIR < T // ROWS)
            def _():
                hs(i + PAIR).start()

    def norm(i):
        r, k = seg(i, ROWS), lax.rem(i, HB)
        wide, scale = norm_of(hb[k])
        cut = [slice(W * q, W * q + W) for q in range(NX)]
        along = sum(jnp.sum(da[q, r] * wide[:, cut[q]], -1, keepdims=True) for q in range(NX))
        along = scale * scale * scale * (along / D)
        parts = [(dy[r, cut[q]].astype(F32) + (scale * da[q, r] - wide[:, cut[q]] * along)).astype(BF) for q in range(NX)]
        for q in range(NX):
            a[r, cut[q]] = parts[q]
            aT[cut[q], r] = parts[q].T
    a0 = fetch(a0T_h, dyT, s_in.at[0])

    def after1(_):
        a0.start()

    def tiles(j):
        k = par(j)
        return [fetch(wd0_h.at[tile_cols(j)], wd.at[k], s_w.at[CORES, k]), fetch(g_h.at[j], da.at[CORES * k], s_w.at[0, k]), fetch(u_h.at[j], da.at[CORES * k + 1], s_w.at[1, k])]

    def before0(_):
        a0.wait()
        start(tiles(jnp.int32(0)))

    def tile0(j):
        k = par(j)

        @pl.when(j + 1 < TILES)
        def _():
            start(tiles(j + 1))
        done(tiles(j))

        def part(r):
            d = dot(a[r], wd[k], NT).astype(BF).astype(F32)
            _, dg, du = hidden(d, da[CORES * k, r], da[CORES * k + 1, r])
            dgb[0, r], dub[0, r] = dg.astype(BF), du.astype(BF)
        sums.gu.free(TILES + j, 0)
        halves(part, GROUP)
        sums.put(TILES + j, 0, dyT[...], dgb[0])
        sums.put(TILES + j, 1, dyT[...], dub[0])
    sums.loop(tile1, (norm_loads, norm), after1, before0, tile0)


def bb(*args):
    tiles = S((TILES, T, W), BF)
    return pl.pallas_call(
        bb_kernel, name="bb",
        out_shape=[S((PAIR, LAYERS, GR, F), BF), S((LAYERS, NY * LANES, D), BF), S((LAYERS, F, D), BF), tiles, tiles, tiles, S((PAIR, SHARDS, GR, F), BF)],
        in_specs=[ANY] * len(args), out_specs=[ANY] * 7,
        scratch_shapes=[V((T, D), BF), V((D, T), BF), V((T, D), BF), V((D, T), BF), V((NX, T, W), F32), slots(GR, F - HEAD), slots(SHARDS, GR, W), slots(SHARDS, GR, W), slots(W, D),
                        slots(T, W), slots(T, W), slots(T, W), slots(W, D), slots(NX, DR, W), V((HB, ROWS, D), BF),
                        DMA((4,)), DMA((2,)), DMA((3, 2)), DMA((3, 2)), DMA((2,)), DMA((NX,)), DMA((HB,))]
        + [s for part in bb_parts() for s in part.scratch()] + Sums().scratch(),
        compiler_params=params(2), cost_estimate=cost(12),
    )(*args)[:2]


def adamw(w, m, v, g):
    m = 0.9 * m + 0.1 * g
    v = 0.95 * v + 0.05 * g * g
    step = m * lax.rsqrt(v + 1e-8) + 0.1 * w
    return (w - 0.02 * step).astype(BF), m, v


def solution(mesh):
    def step(x, dy, *arrays):
        weights, m, v = (arrays[i:i + 3] for i in (0, 3, 6))
        x, dy = x[0], dy[0]
        _, d0, d1, head, g0, u0, act0, h1, a1, a1T, a0T, dyT = fa(x, dy, *weights)
        gu, dn = bb(a1, a1T, dy, dyT, h1, weights[0], weights[1], head, d1.reshape(F, D), a0T, act0, g0, u0, d0.reshape(F, D))
        grads = [gu[0], gu[1], dn[:, :DR]]
        new = [adamw(w.astype(F32), m_, v_, g.astype(F32)) for w, m_, v_, g in zip(weights, m, v, grads)]
        return tuple(one[k] for k in range(3) for one in new)

    states, cut = P(("rep", "r", "s"), None, None), P(None, "s", None)
    return jax.shard_map(step, mesh=mesh, in_specs=(states, states) + (cut,) * 9, out_specs=(P("rep", "s", None),) * 9, check_vma=False)
```
